128 devices in a mesh: emb: 4 (over z), col: 4 (over y), row: 8 (over x, core).
Axes of the slice: x: 4, y: 4, z: 4, core: 2. Of those that a mesh axis runs over, the one named last changes fastest.
Arguments:
- inter_mask: int32 [2048, 65536], P('row', 'col')
- emb_user: bfloat16 [2048, 64], P(('row', 'col'), 'emb')
- emb_item: bfloat16 [65536, 64], P(('col', 'row'), 'emb')
- triples: int32 [4096, 3], replicated
Outputs:
- output 1: bfloat16 [2048, 64], P(('row', 'col'), 'emb')
- output 2: bfloat16 [65536, 64], P(('col', 'row'), 'emb')
- output 3: float32 [4096], replicated
All inputs are finite; a program needn't handle non-finite values.
Results may differ from the reference program's by a relative error of at most 0.0107327.
Values are sent between devices in bfloat16 or wider.
A program may use at most 1 GiB of HBM per device.

```python
import jax
import jax.numpy as jnp
from jax import lax

NUM_USERS = 2048
NUM_ITEMS = 65536
EMB_DIM = 64
NUM_TRIPLES = 4096
NUM_LAYERS = 3
SPARSITY = 8
NUM_GROUPS = 32


def setup_inputs(seed: int = 0) -> dict:
    key = jax.random.key(seed)
    key_list = jax.random.split(key, 10)
    inter_mask = (jax.random.randint(key_list[0], (NUM_USERS, NUM_ITEMS), 0, SPARSITY) == 0).astype(jnp.int32)
    mean_user = jax.random.normal(key_list[1], (EMB_DIM,), jnp.float32)
    mean_item = jax.random.normal(key_list[2], (EMB_DIM,), jnp.float32)
    noise_user = jax.random.normal(key_list[3], (NUM_USERS, EMB_DIM), jnp.float32)
    noise_item = jax.random.normal(key_list[4], (NUM_ITEMS, EMB_DIM), jnp.float32)
    group_user = jax.random.normal(key_list[8], (NUM_GROUPS, EMB_DIM), jnp.float32)
    group_item = jax.random.normal(key_list[9], (NUM_GROUPS, EMB_DIM), jnp.float32)
    user_group = (jnp.arange(NUM_USERS) * NUM_GROUPS) // NUM_USERS
    item_group = (jnp.arange(NUM_ITEMS) * NUM_GROUPS) // NUM_ITEMS
    emb_user = (0.5 * (mean_user[None, :] + 1.5 * group_user[user_group] + noise_user)).astype(jnp.bfloat16)
    emb_item = (0.5 * (mean_item[None, :] + 1.5 * group_item[item_group] + noise_item)).astype(jnp.bfloat16)
    users = jax.random.randint(key_list[5], (NUM_TRIPLES,), 0, NUM_USERS).at[0].set(NUM_USERS - 1)
    pos_items = jax.random.randint(key_list[6], (NUM_TRIPLES,), 0, NUM_ITEMS).at[0].set(NUM_ITEMS - 1)
    neg_items = jax.random.randint(key_list[7], (NUM_TRIPLES,), 0, NUM_ITEMS).at[1].set(0)
    triples = jnp.stack([users, pos_items, neg_items], axis=1).astype(jnp.int32)
    return {"inter_mask": inter_mask, "emb_user": emb_user, "emb_item": emb_item, "triples": triples}


def reference(inter_mask, emb_user, emb_item, triples):
    deg_user = jnp.maximum(jnp.sum(inter_mask, axis=1), 1).astype(jnp.float32)
    deg_item = jnp.maximum(jnp.sum(inter_mask, axis=0), 1).astype(jnp.float32)
    adj_norm = ((lax.rsqrt(deg_user)[:, None] * inter_mask.astype(jnp.float32)) * lax.rsqrt(deg_item)[None, :]).astype(jnp.bfloat16)

    def layer_step(carry, unused):
        user_cur, item_cur, user_acc, item_acc = carry
        user_next = jnp.dot(adj_norm, item_cur, preferred_element_type=jnp.float32).astype(jnp.bfloat16)
        item_next = jnp.dot(adj_norm.T, user_cur, preferred_element_type=jnp.float32).astype(jnp.bfloat16)
        new_carry = (user_next, item_next, user_acc + user_next.astype(jnp.float32), item_acc + item_next.astype(jnp.float32))
        return new_carry, None

    init_state = (emb_user, emb_item, emb_user.astype(jnp.float32), emb_item.astype(jnp.float32))
    carry_out, scan_ys = lax.scan(layer_step, init_state, None, length=NUM_LAYERS)
    final_user = (carry_out[2] / (NUM_LAYERS + 1)).astype(jnp.bfloat16)
    final_item = (carry_out[3] / (NUM_LAYERS + 1)).astype(jnp.bfloat16)
    e_user = jnp.take(final_user, triples[:, 0], axis=0).astype(jnp.float32)
    e_pos = jnp.take(final_item, triples[:, 1], axis=0).astype(jnp.float32)
    e_neg = jnp.take(final_item, triples[:, 2], axis=0).astype(jnp.float32)
    score = jnp.sum(e_user * (e_pos - e_neg), axis=1)
    bpr_loss = jax.nn.softplus(-score)
    return final_user, final_item, bpr_loss
```

```python
import jax
import jax.numpy as jnp
from jax import lax
from jax.experimental import pallas as pl
from jax.experimental.pallas import tpu as pltpu
from jax.sharding import PartitionSpec as P

NUM_LAYERS = 3
MESH = pl.DeviceIdType.MESH
F32 = jnp.float32
BF16 = jnp.bfloat16
EMB = 64
COLS = 16
LANE = 128
CHUNK = 512
ITEMS = 2048
USERS = 256
PEERS = 32
OTHERS = PEERS - 1


def pack_half(top, bot, lane_lo):
    first = jnp.where(lane_lo, top, pltpu.roll(bot, EMB, 1))
    second = jnp.where(lane_lo, pltpu.roll(top, EMB, 1), bot)
    return first, second


def unpack_half(first, second, lane_lo):
    top = jnp.where(lane_lo, first, pltpu.roll(second, EMB, 1))
    bot = jnp.where(lane_lo, pltpu.roll(first, EMB, 1), second)
    return top, bot


def pick_rows(table, ids):
    n = ids.shape[1]
    low = jnp.bitwise_and(ids, 127)
    high = lax.shift_right_arithmetic(ids, 7)
    hot = (lax.broadcasted_iota(jnp.int32, (LANE, n), 0) == low).astype(F32).astype(BF16)
    wide = jnp.dot(table, hot, preferred_element_type=F32)
    high16 = jnp.broadcast_to(high, (COLS, n))
    total = jnp.zeros((COLS, n), F32)
    for blk in range(COLS):
        total = total + jnp.where(high16 == blk, wide[blk * COLS:(blk + 1) * COLS], 0.0)
    return total


def place():
    e = lax.axis_index("emb")
    c = lax.axis_index("col")
    r = lax.axis_index("row")
    return e, c, r, r // 2, r % 2


def device(r, c, e):
    return (e, c, r)


def loop(n, body):
    lax.fori_loop(1, n, lambda j, carry: (body(j), carry)[1], 0)


class Links:
    def __init__(self, send_sem, recv_sem):
        self.send_sem = send_sem
        self.recv_sem = recv_sem

    def send(self, src, dst, phase, target):
        pltpu.make_async_remote_copy(src_ref=src, dst_ref=dst, send_sem=self.send_sem.at[phase],
                                     recv_sem=self.recv_sem.at[phase], device_id=target, device_id_type=MESH).start()

    def wait_recv(self, ref, phase):
        pltpu.make_async_copy(ref, ref, self.recv_sem.at[phase]).wait()

    def wait_send(self, ref, phase):
        pltpu.make_async_copy(ref, ref, self.send_sem.at[phase]).wait()


def greet(target):
    pl.semaphore_signal(pltpu.get_barrier_semaphore(), inc=1, device_id=target, device_id_type=MESH)


def load_kernel(mask_ref, own_ref, other_ref, du_ref, di_ref, m_loc, sems):
    e, c, r, x, k = place()
    loads = []
    for par in (1, 0):
        for xx in range(4):
            row = 2 * xx + jnp.bitwise_xor(k, par)
            off = pl.multiple_of(row * ITEMS + e * CHUNK, CHUNK)
            cp = pltpu.make_async_copy(mask_ref.at[:, pl.ds(off, CHUNK)], m_loc.at[par, xx], sems.at[par * 4 + xx])
            cp.start()
            loads.append((par, xx, cp))
    lanes = jnp.zeros((USERS, LANE), F32)
    for par, xx, cp in loads:
        cp.wait()
        m = m_loc[par, xx].astype(F32)
        (other_ref if par else own_ref)[xx] = m.astype(BF16)
        di_ref[par, :, xx * CHUNK:(xx + 1) * CHUNK] = jnp.sum(m, axis=0, keepdims=True)
        for g in range(4):
            lanes = lanes + m[:, g * LANE:(g + 1) * LANE]
    rows = lax.dot_general(jnp.ones((8, LANE), BF16), lanes.astype(BF16), (((1,), (1,)), ((), ())),
                           preferred_element_type=F32)
    du_ref[...] = rows[0:1]


def degree_kernel(other_ref, du_ref, di_ref, rem_ref, su_ref, si_ref, du, di, send_sem, recv_sem):
    e, c, r, x, k = place()
    q = k * COLS + c * 4 + e
    links = Links(send_sem, recv_sem)

    def q_dev(qq):
        return device(2 * x + qq // COLS, (qq // 4) % 4, qq % 4)

    loop(PEERS, lambda j: greet(q_dev(lax.rem(q + j, PEERS))))
    for j in range(2, 8):
        greet(device(2 * lax.rem(x + j // 2, 4) + j % 2, c, e))
    pl.semaphore_wait(pltpu.get_barrier_semaphore(), OTHERS + 6)
    loop(PEERS, lambda j: links.send(du_ref, du.at[q], 0, q_dev(lax.rem(q + j, PEERS))))
    for j in range(1, 8):
        links.send(di_ref.at[j % 2], di.at[r], 1, device(lax.rem(r + j, 8), c, e))
    links.send(other_ref, rem_ref, 2, device(2 * x + 1 - k, c, e))
    du[q] = du_ref[...]
    di[r] = di_ref[0]
    links.wait_recv(du.at[pl.ds(0, OTHERS)], 0)
    for half in range(2):
        su_ref[half] = jnp.sum(du[half * COLS:(half + 1) * COLS], axis=0)
    links.wait_recv(di.at[pl.ds(0, 7)], 1)
    si_ref[...] = jnp.sum(di[...], axis=0)
    links.wait_recv(rem_ref, 2)
    links.wait_send(du.at[pl.ds(0, OTHERS)], 0)
    links.wait_send(di.at[pl.ds(0, 7)], 1)
    links.wait_send(rem_ref, 2)


def build_kernel(own_ref, rem_ref, su_ref, si_ref, adj_ref):
    k = lax.axis_index("row") % 2
    inv_i = lax.rsqrt(jnp.maximum(si_ref[...], 1.0))
    for source, half in ((own_ref, k), (rem_ref, 1 - k)):
        inv_u = lax.rsqrt(jnp.maximum(su_ref[half], 1.0))
        for rc in range(2):
            col = jnp.broadcast_to(inv_u[:, rc * LANE:(rc + 1) * LANE], (LANE, LANE)).T
            base = pl.multiple_of(half * USERS + rc * LANE, LANE)
            for xx in range(4):
                m = source[xx, rc * LANE:(rc + 1) * LANE, :].astype(F32)
                for g in range(4):
                    lo = xx * CHUNK + g * LANE
                    val = (col * m[:, g * LANE:(g + 1) * LANE]) * inv_i[:, lo:lo + LANE]
                    adj_ref[pl.ds(base, LANE), lo:lo + LANE] = val.astype(BF16)


S_FIN = 0
S_UAG = 1
S_IAG = S_UAG + NUM_LAYERS
S_URS = S_IAG + NUM_LAYERS
S_IRS = S_URS + NUM_LAYERS
N_SEM = S_IRS + NUM_LAYERS


def layers_kernel(adj, ut_v, it_v, ou_ref, oi_ref, pu_ref, uag, iag, usend, urecv, isend, irecv, utp, ei, fin,
                  acc_i, send_sem, recv_sem):
    e, c, r, x, k = place()
    q = k * COLS + c * 4 + e
    links = Links(send_sem, recv_sem)
    send, wait_recv, wait_send = links.send, links.wait_recv, links.wait_send

    def q_dev(qq):
        return device(2 * x + qq // COLS, (qq // 4) % 4, qq % 4)

    def xz_dev(idx):
        return device(2 * (idx // 4) + k, c, idx % 4)

    loop(PEERS, lambda j: greet(q_dev(lax.rem(q + j, PEERS))))
    for j in range(1, 4):
        for dz in range(4):
            greet(device(2 * lax.rem(x + j, 4) + k, c, lax.rem(e + dz, 4)))
    pl.semaphore_wait(pltpu.get_barrier_semaphore(), OTHERS + 12)

    lane_lo = lax.broadcasted_iota(jnp.int32, (8, LANE), 1) < EMB

    def send_uag(layer):
        loop(PEERS, lambda j: send(uag.at[layer, q], uag.at[layer, q], S_UAG + layer, q_dev(lax.rem(q + j, PEERS))))

    def send_iag(layer):
        slot = layer % 2
        for j in (2, 1, 3):
            mine = iag.at[slot, pl.ds(x * 4, 4)]
            send(mine, mine, S_IAG + layer, device(2 * lax.rem(x + j, 4) + k, c, e))

    user0 = ut_v[...].astype(F32)
    packed = jnp.concatenate([user0[0:8], user0[8:COLS]], axis=1)
    uag[0, q] = packed.astype(BF16)
    acc_u = packed
    send_uag(0)
    iag[0, x * 4 + e] = it_v[:, pl.ds(pl.multiple_of(e * CHUNK, CHUNK), CHUNK)]

    def send_i0(j):
        idx = lax.rem(x * 4 + e + j, COLS)
        send(it_v.at[:, pl.ds(pl.multiple_of((idx % 4) * CHUNK, CHUNK), CHUNK)],
             iag.at[0, x * 4 + e], S_IAG, xz_dev(idx))

    loop(COLS, send_i0)

    for layer in range(NUM_LAYERS):
        slot = layer % 2
        wait_recv(uag.at[layer, pl.ds(0, OTHERS)], S_UAG + layer)
        for g in range(4):
            for ee in range(4):
                s0 = (g // 2) * COLS + (g % 2) * 8 + ee
                top, bot = unpack_half(uag[layer, s0].astype(F32), uag[layer, s0 + 4].astype(F32), lane_lo)
                utp[ee * COLS:(ee + 1) * COLS, g * LANE:(g + 1) * LANE] = jnp.concatenate([top, bot], axis=0).astype(BF16)
        if layer >= 2:
            wait_send(irecv.at[0, pl.ds(0, 3)], S_IRS + layer - 2)
        for j in (2, 1, 3, 0):
            xx = lax.rem(x + j, 4)
            part = jnp.dot(utp[...], adj[:, pl.ds(pl.multiple_of(xx * CHUNK, CHUNK), CHUNK)], preferred_element_type=F32)
            if j == 0:
                irecv[slot, x] = part
            else:
                isend[slot, j - 1] = part
                send(isend.at[slot, j - 1], irecv.at[slot, x], S_IRS + layer, device(2 * xx + k, c, e))
        if layer == 0:
            wait_recv(iag.at[0, pl.ds(0, 15)], S_IAG)
        else:
            wait_recv(iag.at[slot, pl.ds(0, 12)], S_IAG + layer)
        part = jnp.zeros((EMB, CHUNK), F32)
        for xx in range(4):
            part = part + lax.dot_general(iag[slot, xx * 4:(xx + 1) * 4].reshape(EMB, CHUNK), adj[:, xx * CHUNK:(xx + 1) * CHUNK], (((1,), (1,)), ((), ())),
                                          preferred_element_type=F32)
        if layer == 0:
            acc_i[...] = iag[0, pl.ds(x * 4, 4)].reshape(EMB, CHUNK).astype(F32)
        if layer >= 1:
            wait_send(urecv.at[pl.ds(0, OTHERS)], S_URS + layer - 1)
        for g in range(4):
            for ee in range(4):
                s0 = (g // 2) * COLS + (g % 2) * 8 + ee
                v = part[ee * COLS:(ee + 1) * COLS, g * LANE:(g + 1) * LANE]
                first, second = pack_half(v[0:8], v[8:COLS], lane_lo)
                usend[s0] = first
                usend[s0 + 4] = second

        def send_u(j, layer=layer):
            qq = lax.rem(q + j, PEERS)
            send(usend.at[qq], urecv.at[q], S_URS + layer, q_dev(qq))

        loop(PEERS, send_u)
        urecv[q] = usend[q]
        wait_recv(urecv.at[pl.ds(0, OTHERS)], S_URS + layer)
        nxt = jnp.sum(urecv[...], axis=0).astype(BF16)
        acc_u = acc_u + nxt.astype(F32)
        if layer + 1 < NUM_LAYERS:
            uag[layer + 1, q] = nxt
            send_uag(layer + 1)
        wait_recv(irecv.at[slot, pl.ds(0, 3)], S_IRS + layer)
        nxt = ((irecv[slot, 0] + irecv[slot, 1]) + (irecv[slot, 2] + irecv[slot, 3])).astype(BF16)
        if layer + 1 < NUM_LAYERS:
            iag[(layer + 1) % 2, pl.ds(x * 4, 4)] = nxt.reshape(4, COLS, CHUNK)
            send_iag(layer + 1)
        acc_i[...] = acc_i[...] + nxt.astype(F32)

    ei[...] = (acc_i[...] / (NUM_LAYERS + 1)).astype(BF16)
    fin[e] = ei[pl.ds(pl.multiple_of(e * COLS, COLS), COLS), :]
    for j in range(1, 4):
        ee = lax.rem(e + j, 4)
        send(ei.at[pl.ds(pl.multiple_of(ee * COLS, COLS), COLS), :], fin.at[e], S_FIN, device(r, c, ee))
    fin_u = (acc_u / (NUM_LAYERS + 1)).astype(BF16)
    pu_ref[...] = fin_u
    fin_u = fin_u.astype(F32)
    ou_ref[...] = jnp.concatenate([fin_u[:, 0:EMB], pltpu.roll(fin_u, EMB, 1)[:, 0:EMB]], axis=0).astype(BF16)
    for layer in range(NUM_LAYERS):
        wait_send(uag.at[layer, pl.ds(0, OTHERS)], S_UAG + layer)
        if layer == 0:
            wait_send(iag.at[0, pl.ds(0, 15)], S_IAG)
        else:
            wait_send(iag.at[layer % 2, pl.ds(0, 12)], S_IAG + layer)
    wait_send(urecv.at[pl.ds(0, OTHERS)], S_URS + NUM_LAYERS - 1)
    wait_send(irecv.at[0, pl.ds(0, 3)], S_IRS + NUM_LAYERS - 2)
    wait_send(irecv.at[0, pl.ds(0, 3)], S_IRS + NUM_LAYERS - 1)
    wait_send(fin.at[pl.ds(0, 3)], S_FIN)
    wait_recv(fin.at[pl.ds(0, 3)], S_FIN)
    for s in range(4):
        oi_ref[:, s * CHUNK:(s + 1) * CHUNK] = fin[s]


def loss_kernel(pu_ref, it_ref, tr_ref, ol_ref, eu, wmat, umat, dsend, drecv, sz, lag, send_sem, recv_sem):
    e, c, r, x, k = place()
    b = r * 4 + c
    links = Links(send_sem, recv_sem)
    send, wait_recv, wait_send = links.send, links.wait_recv, links.wait_send

    def b_dev(bb):
        return device(bb // 4, bb % 4, e)

    loop(PEERS, lambda j: greet(b_dev(lax.rem(b + j, PEERS))))
    for j in range(1, 4):
        greet(device(r, c, lax.rem(e + j, 4)))
    lane_lo = lax.broadcasted_iota(jnp.int32, (8, LANE), 1) < EMB
    for h in range(COLS):
        wmat[h * COLS:(h + 1) * COLS, :] = it_ref[:, h * LANE:(h + 1) * LANE]
    eu[b] = pu_ref[...]
    first_item = (c * 8 + r) * ITEMS

    def differences(t, carry):
        ids = tr_ref[:, pl.ds(pl.multiple_of(t * CHUNK, CHUNK), CHUNK)] - first_item
        diff = pick_rows(wmat[...], ids[1:2]) - pick_rows(wmat[...], ids[2:3])
        for g in range(4):
            dsend[t * 4 + g] = diff[:, g * LANE:(g + 1) * LANE]
        return carry

    lax.fori_loop(0, 8, differences, 0)
    pl.semaphore_wait(pltpu.get_barrier_semaphore(), OTHERS + 3)
    loop(PEERS, lambda j: send(eu.at[b], eu.at[b], 0, b_dev(lax.rem(b + j, PEERS))))

    def send_d(j):
        bb = lax.rem(b + j, PEERS)
        send(dsend.at[bb], drecv.at[b], 1, b_dev(bb))

    loop(PEERS, send_d)
    drecv[b] = dsend[b]
    wait_recv(eu.at[pl.ds(0, OTHERS)], 0)
    for g in range(COLS):
        top, bot = unpack_half(eu[2 * g].astype(F32), eu[2 * g + 1].astype(F32), lane_lo)
        umat[g * COLS:(g + 1) * COLS, :] = jnp.concatenate([top, bot], axis=0).astype(BF16)
    e_user = pick_rows(umat[...], tr_ref[0:1, pl.ds(pl.multiple_of(b * LANE, LANE), LANE)])
    wait_recv(drecv.at[pl.ds(0, OTHERS)], 1)
    sz[e] = jnp.sum(e_user * jnp.sum(drecv[...], axis=0), axis=0, keepdims=True)
    for j in range(1, 4):
        send(sz.at[e], sz.at[e], 2, device(r, c, lax.rem(e + j, 4)))
    wait_recv(sz.at[pl.ds(0, 3)], 2)
    score = (sz[0] + sz[1]) + (sz[2] + sz[3])
    lag[b] = jnp.maximum(-score, 0.0) + jnp.log1p(jnp.exp(-jnp.abs(score)))
    loop(PEERS, lambda j: send(lag.at[b], lag.at[b], 3, b_dev(lax.rem(b + j, PEERS))))
    wait_send(eu.at[pl.ds(0, OTHERS)], 0)
    wait_send(drecv.at[pl.ds(0, OTHERS)], 1)
    wait_send(sz.at[pl.ds(0, 3)], 2)
    wait_recv(lag.at[pl.ds(0, OTHERS)], 3)
    wait_send(lag.at[pl.ds(0, OTHERS)], 3)
    for s in range(PEERS):
        ol_ref[s:s + 1, :] = lag[s]


def call(body, outs, in_specs, scratch, collective_id=None, vmem_mib=24):
    vmem = pl.BlockSpec(memory_space=pltpu.VMEM)
    return pl.pallas_call(
        body,
        out_shape=tuple(jax.ShapeDtypeStruct(shape, dtype) for shape, dtype in outs),
        in_specs=[vmem if s is None else s for s in in_specs],
        out_specs=(vmem,) * len(outs),
        scratch_shapes=scratch,
        compiler_params=pltpu.CompilerParams(
            collective_id=collective_id, has_side_effects=collective_id is not None,
            vmem_limit_bytes=vmem_mib * 1024 * 1024),
        name=body.__name__)


def solution(mesh):
    vm = pltpu.VMEM
    dma = pltpu.SemaphoreType.DMA

    def local_fn(mask_blk, user_sh, item_sh, triples):
        half = ((4, USERS, CHUNK), BF16)
        own, other, du, di = call(
            load_kernel, [half, half, ((1, USERS), F32), ((2, 1, ITEMS), F32)], [pl.BlockSpec(memory_space=pl.ANY)],
            [vm((2, 4, USERS, CHUNK), jnp.int32), dma((8,))], vmem_mib=49)(mask_blk)
        rem, su, si = call(
            degree_kernel, [half, ((2, 1, USERS), F32), ((1, ITEMS), F32)], [None] * 3,
            [vm((PEERS, 1, USERS), F32), vm((8, 1, ITEMS), F32), dma((3,)), dma((3,))], 0)(other, du, di)
        adj, = call(build_kernel, [((CHUNK, ITEMS), BF16)], [None] * 4, [])(own, rem, su, si)
        out_u, out_i, packed_u = call(
            layers_kernel, [((COLS, EMB), BF16), ((COLS, ITEMS), BF16), ((8, LANE), BF16)], [None] * 3,
            [vm((NUM_LAYERS, PEERS, 8, LANE), BF16), vm((2, COLS, COLS, CHUNK), BF16), vm((PEERS, 8, LANE), F32),
             vm((PEERS, 8, LANE), F32), vm((2, 3, EMB, CHUNK), F32), vm((2, 4, EMB, CHUNK), F32), vm((EMB, CHUNK), BF16),
             vm((EMB, CHUNK), BF16), vm((4, COLS, CHUNK), BF16), vm((EMB, CHUNK), F32), dma((N_SEM,)), dma((N_SEM,))],
            1)(adj, user_sh.T, item_sh.T)
        loss, = call(
            loss_kernel, [((PEERS, LANE), F32)], [None] * 3,
            [vm((PEERS, 8, LANE), BF16), vm((USERS, LANE), BF16), vm((USERS, LANE), BF16), vm((PEERS, COLS, LANE), F32),
             vm((PEERS, COLS, LANE), F32), vm((4, 1, LANE), F32), vm((PEERS, 1, LANE), F32), dma((4,)), dma((4,))],
            2)(packed_u, out_i, triples.T)
        return out_u.T, out_i.T, loss.reshape(4096)

    return jax.shard_map(
        local_fn, mesh=mesh,
        in_specs=(P("row", "col"), P(("row", "col"), "emb"), P(("col", "row"), "emb"), P()),
        out_specs=(P(("row", "col"), "emb"), P(("col", "row"), "emb"), P()),
        check_vma=False)
```

```python
import jax
import jax.numpy as jnp
from jax import lax
from jax.experimental import pallas as pl
from jax.experimental.pallas import tpu as pltpu
from jax.sharding import PartitionSpec as P

NUM_LAYERS = 3
MESH = pl.DeviceIdType.MESH
F32 = jnp.float32
BF16 = jnp.bfloat16
EMB = 64
COLS = 16
LANE = 128
CHUNK = 512
ITEMS = 2048
USERS = 256
PEERS = 32
OTHERS = PEERS - 1


def pack_half(top, bot, lane_lo):
    first = jnp.where(lane_lo, top, pltpu.roll(bot, EMB, 1))
    second = jnp.where(lane_lo, pltpu.roll(top, EMB, 1), bot)
    return first, second


def unpack_half(first, second, lane_lo):
    top = jnp.where(lane_lo, first, pltpu.roll(second, EMB, 1))
    bot = jnp.where(lane_lo, pltpu.roll(first, EMB, 1), second)
    return top, bot


def pick_rows(table, ids):
    n = ids.shape[1]
    low = jnp.bitwise_and(ids, 127)
    high = lax.shift_right_arithmetic(ids, 7)
    hot = (lax.broadcasted_iota(jnp.int32, (LANE, n), 0) == low).astype(F32).astype(BF16)
    wide = jnp.dot(table, hot, preferred_element_type=F32)
    high16 = jnp.broadcast_to(high, (COLS, n))
    total = jnp.zeros((COLS, n), F32)
    for blk in range(COLS):
        total = total + jnp.where(high16 == blk, wide[blk * COLS:(blk + 1) * COLS], 0.0)
    return total


def place():
    e = lax.axis_index("emb")
    c = lax.axis_index("col")
    r = lax.axis_index("row")
    return e, c, r, r // 2, r % 2


def device(r, c, e):
    return (e, c, r)


class Links:
    def __init__(self, send_sem, recv_sem):
        self.send_sem = send_sem
        self.recv_sem = recv_sem

    def send(self, src, dst, phase, target):
        pltpu.make_async_remote_copy(src_ref=src, dst_ref=dst, send_sem=self.send_sem.at[phase],
                                     recv_sem=self.recv_sem.at[phase], device_id=target, device_id_type=MESH).start()

    def wait_recv(self, ref, phase):
        pltpu.make_async_copy(ref, ref, self.recv_sem.at[phase]).wait()

    def wait_send(self, ref, phase):
        pltpu.make_async_copy(ref, ref, self.send_sem.at[phase]).wait()


def greet(target):
    pl.semaphore_signal(pltpu.get_barrier_semaphore(), inc=1, device_id=target, device_id_type=MESH)


def load_kernel(mask_ref, own_ref, other_ref, du_ref, di_ref, m_loc, sems):
    e, c, r, x, k = place()
    loads = []
    for par in (1, 0):
        for xx in range(4):
            row = 2 * xx + jnp.bitwise_xor(k, par)
            off = pl.multiple_of(row * ITEMS + e * CHUNK, CHUNK)
            cp = pltpu.make_async_copy(mask_ref.at[:, pl.ds(off, CHUNK)], m_loc.at[par, xx], sems.at[par * 4 + xx])
            cp.start()
            loads.append((par, xx, cp))
    lanes = jnp.zeros((USERS, LANE), F32)
    for par, xx, cp in loads:
        cp.wait()
        m = m_loc[par, xx].astype(F32)
        (other_ref if par else own_ref)[xx] = m.astype(BF16)
        di_ref[par, :, xx * CHUNK:(xx + 1) * CHUNK] = jnp.sum(m, axis=0, keepdims=True)
        for g in range(4):
            lanes = lanes + m[:, g * LANE:(g + 1) * LANE]
    rows = lax.dot_general(jnp.ones((8, LANE), BF16), lanes.astype(BF16), (((1,), (1,)), ((), ())),
                           preferred_element_type=F32)
    du_ref[...] = rows[0:1]


S_MASK, S_DU, S_DI, S_FIN, S_EU, S_D, S_SZ, S_LOSS = range(8)
S_UAG = S_LOSS + 1
S_IAG = S_UAG + NUM_LAYERS
S_URS = S_IAG + NUM_LAYERS
S_IRS = S_URS + NUM_LAYERS
N_SEM = S_IRS + NUM_LAYERS


def far_first(*sizes):
    offsets = [()]
    for size in sizes:
        offsets = [o + (d,) for o in offsets for d in range(size)]
    hops = lambda o: sum(min(d, n - d) for d, n in zip(o[:-1], sizes)) * 2 + o[-1]
    return sorted(offsets[1:], key=hops, reverse=True)


def main_kernel(own_ref, other_ref, du_ref, di_ref, ut_v, it_v, tr_ref, ou_ref, oi_ref, ol_ref,
                rem, adj, du, di, uag, iag, usend, urecv, isend, irecv, utp, ei, fin, acc_i,
                eu, wmat, umat, dsend, drecv, sz, lag, send_sem, recv_sem):
    e, c, r, x, k = place()
    q = k * COLS + c * 4 + e
    b = r * 4 + c
    links = Links(send_sem, recv_sem)
    send, wait_recv, wait_send = links.send, links.wait_recv, links.wait_send
    es = [lax.rem(e + d, 4) for d in range(4)]
    cs = [lax.rem(c + d, 4) for d in range(4)]
    xs = [lax.rem(x + d, 4) for d in range(4)]
    ks = [k, 1 - k]
    partner = device(2 * x + ks[1], c, e)
    q_peers = [(ks[dk] * COLS + cs[dc] * 4 + es[de], device(2 * x + ks[dk], cs[dc], es[de]))
               for dc, de, dk in far_first(4, 4, 2)]
    b_peers = [((2 * xs[dx] + ks[dk]) * 4 + cs[dc], device(2 * xs[dx] + ks[dk], cs[dc], e))
               for dx, dc, dk in far_first(4, 4, 2)]
    xz_peers = [(es[de], device(2 * xs[dx] + k, c, es[de])) for dx, de, _ in far_first(4, 4, 1)]

    for _, target in q_peers:
        greet(target)
    for dx in range(1, 4):
        for de in range(4):
            greet(device(2 * xs[dx] + k, c, es[de]))
        greet(device(2 * xs[dx] + ks[1], c, e))
    pl.semaphore_wait(pltpu.get_barrier_semaphore(), OTHERS + 12 + 3)

    for _, target in q_peers:
        send(du_ref, du.at[q], S_DU, target)
    for dx in (2, 1, 3, 0):
        for dk in range(2):
            if dx or dk:
                send(di_ref.at[dk], di.at[r], S_DI, device(2 * xs[dx] + ks[dk], c, e))
    send(other_ref, rem, S_MASK, partner)
    lane_lo = lax.broadcasted_iota(jnp.int32, (8, LANE), 1) < EMB
    user0 = ut_v[...].astype(F32)
    packed = jnp.concatenate([user0[0:8], user0[8:16]], axis=1)
    uag[0, q] = packed.astype(BF16)
    acc_u = packed

    def send_uag(layer):
        for _, target in q_peers:
            send(uag.at[layer, q], uag.at[layer, q], S_UAG + layer, target)

    def send_iag(layer):
        for j in (2, 1, 3):
            mine = iag.at[layer % 2, pl.ds(x * 4, 4)]
            send(mine, mine, S_IAG + layer, device(2 * xs[j] + k, c, e))

    for ee, target in xz_peers:
        send(it_v.at[:, pl.ds(pl.multiple_of(ee * CHUNK, CHUNK), CHUNK)], iag.at[0, x * 4 + e], S_IAG, target)
    send_uag(0)
    iag[0, x * 4 + e] = it_v[:, pl.ds(pl.multiple_of(e * CHUNK, CHUNK), CHUNK)]
    du[q] = du_ref[...]
    di[r] = di_ref[0]
    wait_recv(du.at[pl.ds(0, OTHERS)], S_DU)
    wait_recv(di.at[pl.ds(0, 7)], S_DI)

    inv_i = lax.rsqrt(jnp.maximum(jnp.sum(di[...], axis=0), 1.0))

    def build(source, target, core):
        deg = jnp.sum(du[pl.ds(core * COLS, COLS)], axis=0)
        inv_u = lax.rsqrt(jnp.maximum(deg, 1.0))
        for rc in range(2):
            rows = slice(rc * LANE, (rc + 1) * LANE)
            col = jnp.broadcast_to(inv_u[:, rows], (LANE, LANE)).T
            for xx in range(4):
                m = source[xx, rows, :].astype(F32)
                for g in range(4):
                    lanes = slice(g * LANE, (g + 1) * LANE)
                    lo = xx * CHUNK + g * LANE
                    target[xx, rows, lanes] = ((col * m[:, lanes]) * inv_i[:, lo:lo + LANE]).astype(BF16)

    build(own_ref, adj, ks[0])
    wait_recv(rem, S_MASK)
    build(rem, rem, ks[1])
    parts = ((adj, ks[0]), (rem, ks[1]))

    def item_partials(layer):
        slot = layer % 2
        wait_recv(uag.at[layer, pl.ds(0, OTHERS)], S_UAG + layer)
        for h, (_, core) in enumerate(parts):
            for g in range(2):
                for ee in range(4):
                    s0 = core * COLS + g * 8 + ee
                    top, bot = unpack_half(uag[layer, s0].astype(F32), uag[layer, s0 + 4].astype(F32), lane_lo)
                    both = jnp.concatenate([top, bot], axis=0).astype(BF16)
                    utp[h, ee * COLS:(ee + 1) * COLS, g * LANE:(g + 1) * LANE] = both
        if layer >= 2:
            wait_send(irecv.at[0, pl.ds(0, 3)], S_IRS + layer - 2)
        for j in (2, 1, 3, 0):
            part = jnp.dot(utp[0], adj[xs[j]], preferred_element_type=F32)
            part = part + jnp.dot(utp[1], rem[xs[j]], preferred_element_type=F32)
            if j == 0:
                irecv[slot, x] = part
            else:
                isend[slot, j - 1] = part
                send(isend.at[slot, j - 1], irecv.at[slot, x], S_IRS + layer, device(2 * xs[j] + k, c, e))

    def user_partials(layer):
        slot = layer % 2
        if layer == 0:
            wait_recv(iag.at[0, pl.ds(0, 15)], S_IAG)
        else:
            wait_recv(iag.at[slot, pl.ds(0, 12)], S_IAG + layer)
        if layer >= 1:
            wait_send(usend.at[pl.ds(0, OTHERS)], S_URS + layer - 1)
        for half, core in parts:
            part = jnp.zeros((EMB, USERS), F32)
            for xx in range(4):
                part = part + lax.dot_general(iag[slot, xx * 4:(xx + 1) * 4].reshape(EMB, CHUNK), half[xx],
                                              (((1,), (1,)), ((), ())), preferred_element_type=F32)
            for g in range(2):
                for ee in range(4):
                    s0 = core * COLS + g * 8 + ee
                    v = part[ee * COLS:(ee + 1) * COLS, g * LANE:(g + 1) * LANE]
                    first, second = pack_half(v[0:8], v[8:16], lane_lo)
                    usend[s0] = first
                    usend[s0 + 4] = second
        for qq, target in q_peers:
            send(usend.at[qq], urecv.at[slot, q], S_URS + layer, target)
        urecv[slot, q] = usend[q]

    def next_users(layer):
        wait_recv(urecv.at[layer % 2, pl.ds(0, OTHERS)], S_URS + layer)
        return jnp.sum(urecv[layer % 2], axis=0).astype(BF16)

    def next_items(layer):
        slot = layer % 2
        wait_recv(irecv.at[slot, pl.ds(0, 3)], S_IRS + layer)
        return ((irecv[slot, 0] + irecv[slot, 1]) + (irecv[slot, 2] + irecv[slot, 3])).astype(BF16)

    for layer in range(NUM_LAYERS):
        last = layer + 1 == NUM_LAYERS
        if last:
            item_partials(layer)
            user_partials(layer)
            item_next = next_items(layer)
            item_sum = acc_i[...] + item_next.astype(F32)
        else:
            user_partials(layer)
            if layer == 0:
                acc_i[...] = iag[0, pl.ds(x * 4, 4)].reshape(EMB, CHUNK).astype(F32)
            item_partials(layer)
            user_next = next_users(layer)
            uag[layer + 1, q] = user_next
            send_uag(layer + 1)
            acc_u = acc_u + user_next.astype(F32)
            item_next = next_items(layer)
            iag[(layer + 1) % 2, pl.ds(x * 4, 4)] = item_next.reshape(4, COLS, CHUNK)
            send_iag(layer + 1)
            acc_i[...] = acc_i[...] + item_next.astype(F32)

    ei[...] = (item_sum / (NUM_LAYERS + 1)).astype(BF16)
    for j in (2, 1, 3):
        send(ei.at[pl.ds(pl.multiple_of(es[j] * COLS, COLS), COLS), :], fin.at[e], S_FIN, device(r, c, es[j]))
    fin[e] = ei[pl.ds(pl.multiple_of(e * COLS, COLS), COLS), :]
    acc_u = acc_u + next_users(NUM_LAYERS - 1).astype(F32)
    fin_u = (acc_u / (NUM_LAYERS + 1)).astype(BF16)
    eu[b] = fin_u
    for _, target in b_peers:
        send(eu.at[b], eu.at[b], S_EU, target)
    fin_u = fin_u.astype(F32)
    ou_ref[...] = jnp.concatenate([fin_u[:, 0:EMB], pltpu.roll(fin_u, EMB, 1)[:, 0:EMB]], axis=0).astype(BF16)
    wait_recv(fin.at[pl.ds(0, 3)], S_FIN)
    for h in range(COLS):
        wmat[h * COLS:(h + 1) * COLS, :] = fin[h // 4, :, (h % 4) * LANE:(h % 4 + 1) * LANE]
    first_item = (c * 8 + r) * ITEMS

    def differences(i, carry):
        row = (r + 4 + i) % 8
        ids = tr_ref[:, pl.ds(pl.multiple_of(row * CHUNK, CHUNK), CHUNK)] - first_item
        diff = pick_rows(wmat[...], ids[1:2]) - pick_rows(wmat[...], ids[2:3])
        for g in range(4):
            dsend[row * 4 + g] = diff[:, g * LANE:(g + 1) * LANE]
        for g in range(4):
            @pl.when(row * 4 + g != b)
            def _():
                send(dsend.at[row * 4 + g], drecv.at[b], S_D, device(row, g, e))
        return carry

    lax.fori_loop(0, 8, differences, 0)
    drecv[b] = dsend[b]
    wait_recv(eu.at[pl.ds(0, OTHERS)], S_EU)
    for g in range(COLS):
        top, bot = unpack_half(eu[2 * g].astype(F32), eu[2 * g + 1].astype(F32), lane_lo)
        umat[g * COLS:(g + 1) * COLS, :] = jnp.concatenate([top, bot], axis=0).astype(BF16)
    e_user = pick_rows(umat[...], tr_ref[0:1, pl.ds(pl.multiple_of(b * LANE, LANE), LANE)])
    wait_recv(drecv.at[pl.ds(0, OTHERS)], S_D)
    sz[e] = jnp.sum(e_user * jnp.sum(drecv[...], axis=0), axis=0, keepdims=True)
    for j in (2, 1, 3):
        send(sz.at[e], sz.at[e], S_SZ, device(r, c, es[j]))
    wait_recv(sz.at[pl.ds(0, 3)], S_SZ)
    score = (sz[0] + sz[1]) + (sz[2] + sz[3])
    lag[b] = jnp.maximum(-score, 0.0) + jnp.log1p(jnp.exp(-jnp.abs(score)))
    for _, target in b_peers:
        send(lag.at[b], lag.at[b], S_LOSS, target)
    for s in range(4):
        oi_ref[:, s * CHUNK:(s + 1) * CHUNK] = fin[s]
    wait_send(rem, S_MASK)
    wait_send(du.at[pl.ds(0, OTHERS)], S_DU)
    wait_send(di.at[pl.ds(0, 7)], S_DI)
    for layer in range(NUM_LAYERS):
        wait_send(uag.at[layer, pl.ds(0, OTHERS)], S_UAG + layer)
        if layer == 0:
            wait_send(iag.at[0, pl.ds(0, 15)], S_IAG)
        else:
            wait_send(iag.at[layer % 2, pl.ds(0, 12)], S_IAG + layer)
    wait_send(usend.at[pl.ds(0, OTHERS)], S_URS + NUM_LAYERS - 1)
    for layer in range(NUM_LAYERS - 2, NUM_LAYERS):
        wait_send(irecv.at[0, pl.ds(0, 3)], S_IRS + layer)
    wait_send(fin.at[pl.ds(0, 3)], S_FIN)
    wait_send(eu.at[pl.ds(0, OTHERS)], S_EU)
    wait_send(drecv.at[pl.ds(0, OTHERS)], S_D)
    wait_send(sz.at[pl.ds(0, 3)], S_SZ)
    wait_send(lag.at[pl.ds(0, OTHERS)], S_LOSS)
    wait_recv(lag.at[pl.ds(0, OTHERS)], S_LOSS)
    for s in range(PEERS):
        ol_ref[s:s + 1, :] = lag[s]


def call(body, outs, in_specs, scratch, collective_id=None, vmem_mib=24):
    vmem = pl.BlockSpec(memory_space=pltpu.VMEM)
    return pl.pallas_call(
        body,
        out_shape=tuple(jax.ShapeDtypeStruct(shape, dtype) for shape, dtype in outs),
        in_specs=[vmem if s is None else s for s in in_specs],
        out_specs=(vmem,) * len(outs),
        scratch_shapes=scratch,
        compiler_params=pltpu.CompilerParams(
            collective_id=collective_id, has_side_effects=collective_id is not None,
            vmem_limit_bytes=vmem_mib * 1024 * 1024),
        name=body.__name__)


def solution(mesh):
    vm = pltpu.VMEM
    dma = pltpu.SemaphoreType.DMA

    def local_fn(mask_blk, user_sh, item_sh, triples):
        half = (4, USERS, CHUNK)
        pieces = (PEERS, 8, LANE)
        panel = (EMB, CHUNK)
        own, other, du, di = call(
            load_kernel, [(half, BF16), (half, BF16), ((1, USERS), F32), ((2, 1, ITEMS), F32)],
            [pl.BlockSpec(memory_space=pl.ANY)], [vm((2,) + half, jnp.int32), dma((8,))], vmem_mib=49)(mask_blk)
        out_u, out_i, loss = call(
            main_kernel, [((COLS, EMB), BF16), ((COLS, ITEMS), BF16), ((PEERS, LANE), F32)], [None] * 7,
            [vm(half, BF16), vm(half, BF16), vm((PEERS, 1, USERS), F32), vm((8, 1, ITEMS), F32),
             vm((NUM_LAYERS,) + pieces, BF16), vm((2, 4 * 4, COLS, CHUNK), BF16), vm(pieces, F32),
             vm((2,) + pieces, F32),
             vm((2, 3) + panel, F32), vm((2, 4) + panel, F32), vm((2, EMB, USERS), BF16), vm(panel, BF16),
             vm((4, COLS, CHUNK), BF16), vm(panel, F32),
             vm(pieces, BF16), vm((USERS, LANE), BF16), vm((USERS, LANE), BF16), vm((PEERS, COLS, LANE), F32),
             vm((PEERS, COLS, LANE), F32), vm((4, 1, LANE), F32), vm((PEERS, 1, LANE), F32),
             dma((N_SEM,)), dma((N_SEM,))],
            0)(own, other, du, di, user_sh.T, item_sh.T, triples.T)
        return out_u.T, out_i.T, loss.reshape(PEERS * LANE)

    return jax.shard_map(
        local_fn, mesh=mesh,
        in_specs=(P("row", "col"), P(("row", "col"), "emb"), P(("col", "row"), "emb"), P()),
        out_specs=(P(("row", "col"), "emb"), P(("col", "row"), "emb"), P()),
        check_vma=False)
```

```python
import jax
import jax.numpy as jnp
from jax import lax
from jax.experimental import pallas as pl
from jax.experimental.pallas import tpu as pltpu
from jax.sharding import PartitionSpec as P

NUM_LAYERS = 3
MESH = pl.DeviceIdType.MESH
F32 = jnp.float32
BF16 = jnp.bfloat16
EMB = 64
COLS = 16
LANE = 128
CHUNK = 512
ITEMS = 2048
USERS = 256
PEERS = 32
OTHERS = PEERS - 1


def pack_half(top, bot, lane_lo):
    first = jnp.where(lane_lo, top, pltpu.roll(bot, EMB, 1))
    second = jnp.where(lane_lo, pltpu.roll(top, EMB, 1), bot)
    return first, second


def unpack_half(first, second, lane_lo):
    top = jnp.where(lane_lo, first, pltpu.roll(second, EMB, 1))
    bot = jnp.where(lane_lo, pltpu.roll(first, EMB, 1), second)
    return top, bot


def pick_rows(table, ids):
    n = ids.shape[1]
    low = jnp.bitwise_and(ids, 127)
    high = lax.shift_right_arithmetic(ids, 7)
    hot = (lax.broadcasted_iota(jnp.int32, (LANE, n), 0) == low).astype(F32).astype(BF16)
    wide = jnp.dot(table, hot, preferred_element_type=F32)
    high16 = jnp.broadcast_to(high, (COLS, n))
    total = jnp.zeros((COLS, n), F32)
    for blk in range(COLS):
        total = total + jnp.where(high16 == blk, wide[blk * COLS:(blk + 1) * COLS], 0.0)
    return total


def place():
    e = lax.axis_index("emb")
    c = lax.axis_index("col")
    r = lax.axis_index("row")
    return e, c, r, r // 2, r % 2


def device(r, c, e):
    return (e, c, r)


class Links:
    def __init__(self, send_sem, recv_sem):
        self.send_sem = send_sem
        self.recv_sem = recv_sem

    def send(self, src, dst, phase, target):
        pltpu.make_async_remote_copy(src_ref=src, dst_ref=dst, send_sem=self.send_sem.at[phase],
                                     recv_sem=self.recv_sem.at[phase], device_id=target, device_id_type=MESH).start()

    def wait_recv(self, ref, phase):
        pltpu.make_async_copy(ref, ref, self.recv_sem.at[phase]).wait()

    def wait_send(self, ref, phase):
        pltpu.make_async_copy(ref, ref, self.send_sem.at[phase]).wait()


def greet(target):
    pl.semaphore_signal(pltpu.get_barrier_semaphore(), inc=1, device_id=target, device_id_type=MESH)


def load_kernel(mask_ref, own_ref, other_ref, du_ref, di_ref, m_loc, sems):
    e, c, r, x, k = place()
    loads = []
    for par in (1, 0):
        for xx in range(4):
            row = 2 * xx + jnp.bitwise_xor(k, par)
            off = pl.multiple_of(row * ITEMS + e * CHUNK, CHUNK)
            cp = pltpu.make_async_copy(mask_ref.at[:, pl.ds(off, CHUNK)], m_loc.at[par, xx], sems.at[par * 4 + xx])
            cp.start()
            loads.append((par, xx, cp))
    lanes = jnp.zeros((USERS, LANE), F32)
    for par, xx, cp in loads:
        cp.wait()
        m = m_loc[par, xx].astype(F32)
        (other_ref if par else own_ref)[xx] = m.astype(BF16)
        di_ref[par, :, xx * CHUNK:(xx + 1) * CHUNK] = jnp.sum(m, axis=0, keepdims=True)
        for g in range(4):
            lanes = lanes + m[:, g * LANE:(g + 1) * LANE]
    rows = lax.dot_general(jnp.ones((8, LANE), BF16), lanes.astype(BF16), (((1,), (1,)), ((), ())),
                           preferred_element_type=F32)
    du_ref[...] = rows[0:1]


S_MASK, S_DU, S_DI, S_EU, S_D, S_LOSS, S_FIN = range(7)
S_UAG = S_FIN + NUM_LAYERS
S_IAG = S_UAG + NUM_LAYERS
S_URS = S_IAG + NUM_LAYERS
S_IRS = S_URS + NUM_LAYERS
N_SEM = S_IRS + NUM_LAYERS


def far_first(*sizes):
    offsets = [()]
    for size in sizes:
        offsets = [o + (d,) for o in offsets for d in range(size)]
    hops = lambda o: sum(min(d, n - d) for d, n in zip(o[:-1], sizes)) * 2 + o[-1]
    return sorted(offsets[1:], key=hops, reverse=True)


def main_kernel(own_ref, other_ref, du_ref, di_ref, ut_v, it_v, tr_ref, ou_ref, oi_ref, ol_ref,
                rem, adj, du, di, uag, iag, usend, urecv, isend, irecv, utp, ib, frecv, fin,
                eu, wmat, umat, dsend, drecv, lag, send_sem, recv_sem):
    e, c, r, x, k = place()
    q = k * COLS + c * 4 + e
    b = r * 4 + c
    links = Links(send_sem, recv_sem)
    send, wait_recv, wait_send = links.send, links.wait_recv, links.wait_send
    es = [lax.rem(e + d, 4) for d in range(4)]
    cs = [lax.rem(c + d, 4) for d in range(4)]
    xs = [lax.rem(x + d, 4) for d in range(4)]
    ks = [k, 1 - k]
    partner = device(2 * x + ks[1], c, e)
    q_peers = [(ks[dk] * COLS + cs[dc] * 4 + es[de], device(2 * x + ks[dk], cs[dc], es[de]))
               for dc, de, dk in far_first(4, 4, 2)]
    b_peers = [((2 * xs[dx] + ks[dk]) * 4 + cs[dc], device(2 * xs[dx] + ks[dk], cs[dc], e))
               for dx, dc, dk in far_first(4, 4, 2)]
    all_peers = [device(2 * xs[dx] + ks[dk], cs[dc], es[de]) for dx, dc, de, dk in far_first(4, 4, 4, 2)]
    xz_peers = [(es[de], device(2 * xs[dx] + k, c, es[de])) for dx, de, _ in far_first(4, 4, 1)]

    for _, target in q_peers:
        greet(target)
    for dx in range(1, 4):
        for de in range(4):
            greet(device(2 * xs[dx] + k, c, es[de]))
        greet(device(2 * xs[dx] + ks[1], c, e))
    pl.semaphore_wait(pltpu.get_barrier_semaphore(), OTHERS + 12 + 3)

    for _, target in q_peers:
        send(du_ref, du.at[q], S_DU, target)
    for dx in (2, 1, 3, 0):
        for dk in range(2):
            if dx or dk:
                send(di_ref.at[dk], di.at[r], S_DI, device(2 * xs[dx] + ks[dk], c, e))
    send(other_ref, rem, S_MASK, partner)
    lane_lo = lax.broadcasted_iota(jnp.int32, (8, LANE), 1) < EMB
    user0 = ut_v[...].astype(F32)
    packed = jnp.concatenate([user0[0:8], user0[8:16]], axis=1)
    uag[0, q] = packed.astype(BF16)
    acc_u = packed

    def send_uag(layer):
        for _, target in q_peers:
            send(uag.at[layer, q], uag.at[layer, q], S_UAG + layer, target)

    def send_iag(layer):
        for j in (2, 1, 3):
            mine = iag.at[layer % 2, pl.ds(x * 4, 4)]
            send(mine, mine, S_IAG + layer, device(2 * xs[j] + k, c, e))

    for ee, target in xz_peers:
        send(it_v.at[:, pl.ds(pl.multiple_of(ee * CHUNK, CHUNK), CHUNK)], iag.at[0, x * 4 + e], S_IAG, target)
    send_uag(0)
    iag[0, x * 4 + e] = it_v[:, pl.ds(pl.multiple_of(e * CHUNK, CHUNK), CHUNK)]
    du[q] = du_ref[...]
    di[r] = di_ref[0]
    wait_recv(du.at[pl.ds(0, OTHERS)], S_DU)
    wait_recv(di.at[pl.ds(0, 7)], S_DI)

    inv_i = lax.rsqrt(jnp.maximum(jnp.sum(di[...], axis=0), 1.0))

    def build(source, target, core):
        deg = jnp.sum(du[pl.ds(core * COLS, COLS)], axis=0)
        inv_u = lax.rsqrt(jnp.maximum(deg, 1.0))
        for rc in range(2):
            rows = slice(rc * LANE, (rc + 1) * LANE)
            col = jnp.broadcast_to(inv_u[:, rows], (LANE, LANE)).T
            for xx in range(4):
                m = source[xx, rows, :].astype(F32)
                for g in range(4):
                    lanes = slice(g * LANE, (g + 1) * LANE)
                    lo = xx * CHUNK + g * LANE
                    target[xx, rows, lanes] = ((col * m[:, lanes]) * inv_i[:, lo:lo + LANE]).astype(BF16)

    build(own_ref, adj, ks[0])
    wait_recv(rem, S_MASK)
    build(rem, rem, ks[1])
    parts = ((adj, ks[0]), (rem, ks[1]))

    def item_partials(layer):
        slot = layer % 2
        wait_recv(uag.at[layer, pl.ds(0, OTHERS)], S_UAG + layer)
        for h, (_, core) in enumerate(parts):
            for g in range(2):
                for ee in range(4):
                    s0 = core * COLS + g * 8 + ee
                    top, bot = unpack_half(uag[layer, s0].astype(F32), uag[layer, s0 + 4].astype(F32), lane_lo)
                    both = jnp.concatenate([top, bot], axis=0).astype(BF16)
                    utp[h, ee * COLS:(ee + 1) * COLS, g * LANE:(g + 1) * LANE] = both
        if layer >= 1:
            wait_send(isend.at[pl.ds(0, 3)], S_IRS + layer - 1)
        for j in (2, 1, 3, 0):
            part = jnp.dot(utp[0], adj[xs[j]], preferred_element_type=F32)
            isend[j] = (part + jnp.dot(utp[1], rem[xs[j]], preferred_element_type=F32)).reshape(4, COLS, CHUNK)
            if j and layer + 1 < NUM_LAYERS:
                send(isend.at[j], irecv.at[slot, j - 1], S_IRS + layer, device(2 * xs[j] + k, c, e))
            elif layer + 1 == NUM_LAYERS:
                for de in (2, 1, 3, 0):
                    if j or de:
                        send(isend.at[j, es[de]], frecv.at[x * 4 + e], S_IRS + layer, device(2 * xs[j] + k, c, es[de]))

    def user_partials(layer):
        slot = layer % 2
        if layer == 0:
            wait_recv(iag.at[0, pl.ds(0, 15)], S_IAG)
        else:
            wait_recv(iag.at[slot, pl.ds(0, 12)], S_IAG + layer)
        if layer >= 1:
            wait_send(usend.at[pl.ds(0, OTHERS)], S_URS + layer - 1)
        for half, core in parts:
            part = jnp.zeros((EMB, USERS), F32)
            for xx in range(4):
                part = part + lax.dot_general(iag[slot, xx * 4:(xx + 1) * 4].reshape(EMB, CHUNK), half[xx],
                                              (((1,), (1,)), ((), ())), preferred_element_type=F32)
            for g in range(2):
                for ee in range(4):
                    s0 = core * COLS + g * 8 + ee
                    v = part[ee * COLS:(ee + 1) * COLS, g * LANE:(g + 1) * LANE]
                    first, second = pack_half(v[0:8], v[8:16], lane_lo)
                    usend[s0] = first
                    usend[s0 + 4] = second
        for qq, target in q_peers:
            send(usend.at[qq], urecv.at[slot, q], S_URS + layer, target)
        urecv[slot, q] = usend[q]

    def next_users(layer):
        wait_recv(urecv.at[layer % 2, pl.ds(0, OTHERS)], S_URS + layer)
        return jnp.sum(urecv[layer % 2], axis=0).astype(BF16)

    def next_items(layer):
        slot = layer % 2
        wait_recv(irecv.at[slot], S_IRS + layer)
        return ((isend[0] + irecv[slot, 0]) + (irecv[slot, 1] + irecv[slot, 2])).astype(BF16)

    for layer in range(NUM_LAYERS - 1):
        item_partials(layer)
        user_partials(layer)
        user_next = next_users(layer)
        uag[layer + 1, q] = user_next
        send_uag(layer + 1)
        acc_u = acc_u + user_next.astype(F32)
        iag[(layer + 1) % 2, pl.ds(x * 4, 4)] = next_items(layer)
        send_iag(layer + 1)
        for j in (2, 1, 3):
            send(iag.at[(layer + 1) % 2, x * 4 + es[j]], ib.at[layer, e], S_FIN + layer, device(r, c, es[j]))
        ib[layer, e] = iag[(layer + 1) % 2, x * 4 + e]

    final = NUM_LAYERS - 1
    item_partials(final)
    frecv[x * 4 + e] = isend[0, e]
    user_partials(final)
    for layer in range(final):
        wait_recv(ib.at[layer, pl.ds(0, 3)], S_FIN + layer)
    item_sums = []
    for s in range(4):
        item_sum = it_v[:, s * CHUNK:(s + 1) * CHUNK].astype(F32)
        for layer in range(final):
            item_sum = item_sum + ib[layer, s].astype(F32)
        item_sums.append(item_sum)
    acc_u = acc_u + next_users(final).astype(F32)
    fin_u = (acc_u / (NUM_LAYERS + 1)).astype(BF16)
    eu[b] = fin_u
    for _, target in b_peers:
        send(eu.at[b], eu.at[b], S_EU, target)
    fin_u = fin_u.astype(F32)
    ou_ref[...] = jnp.concatenate([fin_u[:, 0:EMB], pltpu.roll(fin_u, EMB, 1)[:, 0:EMB]], axis=0).astype(BF16)
    wait_recv(frecv.at[pl.ds(0, 15)], S_IRS + final)
    for s in range(4):
        item_next = ((frecv[s] + frecv[4 + s]) + (frecv[4 * 2 + s] + frecv[4 * 3 + s])).astype(BF16)
        fin[s] = ((item_sums[s] + item_next.astype(F32)) / (NUM_LAYERS + 1)).astype(BF16)
    for h in range(COLS):
        wmat[h * COLS:(h + 1) * COLS, :] = fin[h // 4, :, (h % 4) * LANE:(h % 4 + 1) * LANE]
    first_item = (c * 8 + r) * ITEMS

    def differences(i, carry):
        row = (r + 4 + i) % 8
        ids = tr_ref[:, pl.ds(pl.multiple_of(row * CHUNK, CHUNK), CHUNK)] - first_item
        diff = pick_rows(wmat[...], ids[1:2]) - pick_rows(wmat[...], ids[2:3])
        for g in range(4):
            dsend[row * 4 + g] = diff[:, g * LANE:(g + 1) * LANE]
        for g in range(4):
            @pl.when(row * 4 + g != b)
            def _():
                send(dsend.at[row * 4 + g], drecv.at[b], S_D, device(row, g, e))
        return carry

    lax.fori_loop(0, 8, differences, 0)
    drecv[b] = dsend[b]
    wait_recv(eu.at[pl.ds(0, OTHERS)], S_EU)
    for g in range(COLS):
        top, bot = unpack_half(eu[2 * g].astype(F32), eu[2 * g + 1].astype(F32), lane_lo)
        umat[g * COLS:(g + 1) * COLS, :] = jnp.concatenate([top, bot], axis=0).astype(BF16)
    e_user = pick_rows(umat[...], tr_ref[0:1, pl.ds(pl.multiple_of(b * LANE, LANE), LANE)])
    wait_recv(drecv.at[pl.ds(0, OTHERS)], S_D)
    mine = e * PEERS + b
    lag[mine] = jnp.sum(e_user * jnp.sum(drecv[...], axis=0), axis=0, keepdims=True)
    for target in all_peers:
        send(lag.at[mine], lag.at[mine], S_LOSS, target)
    for s in range(4):
        oi_ref[:, s * CHUNK:(s + 1) * CHUNK] = fin[s]
    wait_send(rem, S_MASK)
    wait_send(du.at[pl.ds(0, OTHERS)], S_DU)
    wait_send(di.at[pl.ds(0, 7)], S_DI)
    for layer in range(NUM_LAYERS):
        wait_send(uag.at[layer, pl.ds(0, OTHERS)], S_UAG + layer)
        if layer == 0:
            wait_send(iag.at[0, pl.ds(0, 15)], S_IAG)
        else:
            wait_send(iag.at[layer % 2, pl.ds(0, 12)], S_IAG + layer)
    wait_send(usend.at[pl.ds(0, OTHERS)], S_URS + NUM_LAYERS - 1)
    wait_send(frecv.at[pl.ds(0, 15)], S_IRS + final)
    for layer in range(final):
        wait_send(ib.at[layer, pl.ds(0, 3)], S_FIN + layer)
    wait_send(eu.at[pl.ds(0, OTHERS)], S_EU)
    wait_send(drecv.at[pl.ds(0, OTHERS)], S_D)
    wait_send(lag.at[pl.ds(0, 4 * PEERS - 1)], S_LOSS)
    wait_recv(lag.at[pl.ds(0, 4 * PEERS - 1)], S_LOSS)
    for s in range(PEERS):
        ol_ref[s:s + 1, :] = (lag[s] + lag[s + PEERS]) + (lag[s + 2 * PEERS] + lag[s + 3 * PEERS])
    score = ol_ref[...]
    ol_ref[...] = jnp.maximum(-score, 0.0) + jnp.log1p(jnp.exp(-jnp.abs(score)))


def emit_kernel(ou, oi, ol, ou_ref, oi_ref, ol_ref, sems):
    copies = [pltpu.make_async_copy(a, b, sems.at[i]) for i, (a, b) in enumerate(((oi, oi_ref), (ou, ou_ref), (ol, ol_ref)))]
    for cp in copies:
        cp.start()
    for cp in copies:
        cp.wait()


def call(body, outs, in_specs, scratch, collective_id=None, vmem_mib=24, out_spec=None):
    vmem = pl.BlockSpec(memory_space=pltpu.VMEM)
    return pl.pallas_call(
        body,
        out_shape=tuple(jax.ShapeDtypeStruct(shape, dtype) for shape, dtype in outs),
        in_specs=[vmem if s is None else s for s in in_specs],
        out_specs=(out_spec or vmem,) * len(outs),
        scratch_shapes=scratch,
        compiler_params=pltpu.CompilerParams(
            collective_id=collective_id, has_side_effects=collective_id is not None,
            vmem_limit_bytes=vmem_mib * 1024 * 1024),
        name=body.__name__)


def solution(mesh):
    vm = pltpu.VMEM
    dma = pltpu.SemaphoreType.DMA

    def local_fn(mask_blk, user_sh, item_sh, triples):
        half = (4, USERS, CHUNK)
        pieces = (PEERS, 8, LANE)
        chunk = (4, COLS, CHUNK)
        own, other, du, di = call(
            load_kernel, [(half, BF16), (half, BF16), ((1, USERS), F32), ((2, 1, ITEMS), F32)],
            [pl.BlockSpec(memory_space=pl.ANY)], [vm((2,) + half, jnp.int32), dma((8,))], vmem_mib=49)(mask_blk)
        results = [((COLS, EMB), BF16), ((COLS, ITEMS), BF16), ((PEERS, LANE), F32)]
        made = call(
            main_kernel, results, [None] * 7,
            [vm(half, BF16), vm(half, BF16), vm((PEERS, 1, USERS), F32), vm((8, 1, ITEMS), F32),
             vm((NUM_LAYERS,) + pieces, BF16), vm((2, 4 * 4, COLS, CHUNK), BF16), vm(pieces, F32),
             vm((2,) + pieces, F32),
             vm((4,) + chunk, F32), vm((2, 3) + chunk, F32), vm((2, EMB, USERS), BF16),
             vm((NUM_LAYERS - 1,) + chunk, BF16), vm((4 * 4, COLS, CHUNK), F32), vm(chunk, BF16),
             vm(pieces, BF16), vm((USERS, LANE), BF16), vm((USERS, LANE), BF16), vm((PEERS, COLS, LANE), F32),
             vm((PEERS, COLS, LANE), F32), vm((4 * PEERS, 1, LANE), F32),
             dma((N_SEM,)), dma((N_SEM,))],
            0)(own, other, du, di, user_sh.T, item_sh.T, triples.T)
        out_u, out_i, loss = call(emit_kernel, results, [None] * 3, [dma((3,))], out_spec=pl.BlockSpec(memory_space=pl.ANY))(*made)
        return out_u.T, out_i.T, loss.reshape(PEERS * LANE)

    return jax.shard_map(
        local_fn, mesh=mesh,
        in_specs=(P("row", "col"), P(("row", "col"), "emb"), P(("col", "row"), "emb"), P()),
        out_specs=(P(("row", "col"), "emb"), P(("col", "row"), "emb"), P()),
        check_vma=False)
```

```python
import jax
import jax.numpy as jnp
from jax import lax
from jax.experimental import pallas as pl
from jax.experimental.pallas import tpu as pltpu
from jax.sharding import PartitionSpec as P

NUM_LAYERS = 3
MESH = pl.DeviceIdType.MESH
F32 = jnp.float32
BF16 = jnp.bfloat16
EMB = 64
COLS = 16
LANE = 128
CHUNK = 512
ITEMS = 2048
USERS = 256
PEERS = 32
OTHERS = PEERS - 1


def pack_half(top, bot, lane_lo):
    first = jnp.where(lane_lo, top, pltpu.roll(bot, EMB, 1))
    second = jnp.where(lane_lo, pltpu.roll(top, EMB, 1), bot)
    return first, second


def unpack_half(first, second, lane_lo):
    top = jnp.where(lane_lo, first, pltpu.roll(second, EMB, 1))
    bot = jnp.where(lane_lo, pltpu.roll(first, EMB, 1), second)
    return top, bot


def pick_rows(table, ids):
    n = ids.shape[1]
    low = jnp.bitwise_and(ids, USERS - 1)
    high = jnp.broadcast_to(lax.shift_right_arithmetic(ids, 8), (COLS, n))
    hot = (lax.broadcasted_iota(jnp.int32, (USERS, n), 0) == low).astype(F32).astype(BF16)
    wide = jnp.dot(table, hot, preferred_element_type=F32)
    total = jnp.zeros((COLS, n), F32)
    for blk in range(8):
        total = jnp.where(high == blk, wide[blk * COLS:(blk + 1) * COLS], total)
    return total


def place():
    e = lax.axis_index("emb")
    c = lax.axis_index("col")
    r = lax.axis_index("row")
    return e, c, r, r // 2, r % 2


def device(r, c, e):
    return (e, c, r)


class Links:
    def __init__(self, send_sem, recv_sem):
        self.send_sem = send_sem
        self.recv_sem = recv_sem

    def send(self, src, dst, phase, target):
        pltpu.make_async_remote_copy(src_ref=src, dst_ref=dst, send_sem=self.send_sem.at[phase],
                                     recv_sem=self.recv_sem.at[phase], device_id=target, device_id_type=MESH).start()

    def wait_recv(self, ref, phase):
        pltpu.make_async_copy(ref, ref, self.recv_sem.at[phase]).wait()

    def wait_send(self, ref, phase):
        pltpu.make_async_copy(ref, ref, self.send_sem.at[phase]).wait()


def greet(target):
    pl.semaphore_signal(pltpu.get_barrier_semaphore(), inc=1, device_id=target, device_id_type=MESH)


def load_kernel(mask_ref, own_ref, other_ref, du_ref, di_ref, m_loc, sems):
    e, c, r, x, k = place()
    loads = []
    for par in (1, 0):
        for xx in range(4):
            row = 2 * xx + jnp.bitwise_xor(k, par)
            off = pl.multiple_of(row * ITEMS + e * CHUNK, CHUNK)
            cp = pltpu.make_async_copy(mask_ref.at[:, pl.ds(off, CHUNK)], m_loc.at[par, xx], sems.at[par * 4 + xx])
            cp.start()
            loads.append((par, xx, cp))
    lanes = jnp.zeros((USERS, LANE), F32)
    for par, xx, cp in loads:
        cp.wait()
        m = m_loc[par, xx].astype(F32)
        (other_ref if par else own_ref)[xx] = m.astype(BF16)
        di_ref[par, :, xx * CHUNK:(xx + 1) * CHUNK] = jnp.sum(m, axis=0, keepdims=True)
        for g in range(4):
            lanes = lanes + m[:, g * LANE:(g + 1) * LANE]
    rows = lax.dot_general(jnp.ones((8, LANE), BF16), lanes.astype(BF16), (((1,), (1,)), ((), ())),
                           preferred_element_type=F32)
    du_ref[...] = rows[0:1]


S_MASK, S_DU, S_DI, S_EU, S_D, S_LOSS, S_FIN = range(7)
S_UAG = S_FIN + NUM_LAYERS
S_IAG = S_UAG + NUM_LAYERS
S_URS = S_IAG + NUM_LAYERS
S_IRS = S_URS + NUM_LAYERS
N_SEM = S_IRS + NUM_LAYERS


def far_first(*sizes):
    offsets = [()]
    for size in sizes:
        offsets = [o + (d,) for o in offsets for d in range(size)]
    hops = lambda o: sum(min(d, n - d) for d, n in zip(o[:-1], sizes)) * 2 + o[-1]
    return sorted(offsets[1:], key=hops, reverse=True)


def main_kernel(own_ref, other_ref, du_ref, di_ref, ut_v, it_v, tr_ref, ou_ref, oi_ref, ol_ref,
                rem, adj, du, di, uag, iag, usend, urecv, isend, irecv, utp, ib, frecv, fin,
                eu, wmat, umat, dsend, drecv, lag, send_sem, recv_sem):
    e, c, r, x, k = place()
    q = k * COLS + c * 4 + e
    b = r * 4 + c
    links = Links(send_sem, recv_sem)
    send, wait_recv, wait_send = links.send, links.wait_recv, links.wait_send
    es = [lax.rem(e + d, 4) for d in range(4)]
    cs = [lax.rem(c + d, 4) for d in range(4)]
    xs = [lax.rem(x + d, 4) for d in range(4)]
    ks = [k, 1 - k]
    partner = device(2 * x + ks[1], c, e)
    q_peers = [(ks[dk] * COLS + cs[dc] * 4 + es[de], device(2 * x + ks[dk], cs[dc], es[de]))
               for dc, de, dk in far_first(4, 4, 2)]
    b_peers = [((2 * xs[dx] + ks[dk]) * 4 + cs[dc], device(2 * xs[dx] + ks[dk], cs[dc], e))
               for dx, dc, dk in far_first(4, 4, 2)]
    all_peers = [device(2 * xs[dx] + ks[dk], cs[dc], es[de]) for dx, dc, de, dk in far_first(4, 4, 4, 2)]
    xz_peers = [(es[de], device(2 * xs[dx] + k, c, es[de])) for dx, de, _ in far_first(4, 4, 1)]

    for _, target in q_peers:
        greet(target)
    for dx in range(1, 4):
        for de in range(4):
            greet(device(2 * xs[dx] + k, c, es[de]))
        greet(device(2 * xs[dx] + ks[1], c, e))
    pl.semaphore_wait(pltpu.get_barrier_semaphore(), OTHERS + 12 + 3)

    for _, target in q_peers:
        send(du_ref, du.at[q], S_DU, target)
    for dx in (2, 1, 3, 0):
        for dk in range(2):
            if dx or dk:
                send(di_ref.at[dk], di.at[r], S_DI, device(2 * xs[dx] + ks[dk], c, e))
    send(other_ref, rem, S_MASK, partner)
    lane_lo = lax.broadcasted_iota(jnp.int32, (8, LANE), 1) < EMB
    user0 = ut_v[...].astype(F32)
    packed = jnp.concatenate([user0[0:8], user0[8:16]], axis=1)
    uag[0, q] = packed.astype(BF16)
    acc_u = packed

    def send_uag(layer):
        for _, target in q_peers:
            send(uag.at[layer, q], uag.at[layer, q], S_UAG + layer, target)

    def send_iag(layer):
        for j in (2, 1, 3):
            mine = iag.at[layer % 2, pl.ds(x * 4, 4)]
            send(mine, mine, S_IAG + layer, device(2 * xs[j] + k, c, e))

    for ee, target in xz_peers:
        send(it_v.at[:, pl.ds(pl.multiple_of(ee * CHUNK, CHUNK), CHUNK)], iag.at[0, x * 4 + e], S_IAG, target)
    send_uag(0)
    iag[0, x * 4 + e] = it_v[:, pl.ds(pl.multiple_of(e * CHUNK, CHUNK), CHUNK)]
    du[q] = du_ref[...]
    di[r] = di_ref[0]
    wait_recv(du.at[pl.ds(0, OTHERS)], S_DU)
    wait_recv(di.at[pl.ds(0, 7)], S_DI)

    inv_i = lax.rsqrt(jnp.maximum(jnp.sum(di[...], axis=0), 1.0))

    def build(source, target, core):
        deg = jnp.sum(du[pl.ds(core * COLS, COLS)], axis=0)
        inv_u = lax.rsqrt(jnp.maximum(deg, 1.0))
        for rc in range(2):
            rows = slice(rc * LANE, (rc + 1) * LANE)
            col = jnp.broadcast_to(inv_u[:, rows], (LANE, LANE)).T
            for xx in range(4):
                for g in range(4):
                    lanes = slice(g * LANE, (g + 1) * LANE)
                    lo = xx * CHUNK + g * LANE
                    m = source[xx, rows, lanes].astype(F32)
                    target[xx, rows, lanes] = ((col * m) * inv_i[:, lo:lo + LANE]).astype(BF16)

    build(own_ref, adj, ks[0])
    wait_recv(rem, S_MASK)
    build(rem, rem, ks[1])
    parts = ((adj, ks[0]), (rem, ks[1]))

    def item_partials(layer):
        slot = layer % 2
        wait_recv(uag.at[layer, pl.ds(0, OTHERS)], S_UAG + layer)
        for h, (_, core) in enumerate(parts):
            for g in range(2):
                for ee in range(4):
                    s0 = core * COLS + g * 8 + ee
                    top, bot = unpack_half(uag[layer, s0].astype(F32), uag[layer, s0 + 4].astype(F32), lane_lo)
                    both = jnp.concatenate([top, bot], axis=0).astype(BF16)
                    utp[h, ee * COLS:(ee + 1) * COLS, g * LANE:(g + 1) * LANE] = both
        if layer >= 1:
            wait_send(isend.at[pl.ds(0, 3)], S_IRS + layer - 1)
        for j in (2, 1, 3, 0):
            part = jnp.dot(utp[0], adj[xs[j]], preferred_element_type=F32)
            isend[j] = (part + jnp.dot(utp[1], rem[xs[j]], preferred_element_type=F32)).reshape(4, COLS, CHUNK)
            if j and layer + 1 < NUM_LAYERS:
                send(isend.at[j], irecv.at[slot, j - 1], S_IRS + layer, device(2 * xs[j] + k, c, e))
            elif layer + 1 == NUM_LAYERS:
                for de in (2, 1, 3, 0):
                    if j or de:
                        send(isend.at[j, es[de]], frecv.at[x * 4 + e], S_IRS + layer, device(2 * xs[j] + k, c, es[de]))

    def user_partials(layer):
        slot = layer % 2
        if layer == 0:
            wait_recv(iag.at[0, pl.ds(0, 15)], S_IAG)
        else:
            wait_recv(iag.at[slot, pl.ds(0, 12)], S_IAG + layer)
        if layer >= 1:
            wait_send(usend.at[pl.ds(0, OTHERS)], S_URS + layer - 1)
        for half, core in parts:
            part = jnp.zeros((EMB, USERS), F32)
            for xx in range(4):
                part = part + lax.dot_general(iag[slot, xx * 4:(xx + 1) * 4].reshape(EMB, CHUNK), half[xx],
                                              (((1,), (1,)), ((), ())), preferred_element_type=F32)
            for g in range(2):
                for ee in range(4):
                    s0 = core * COLS + g * 8 + ee
                    v = part[ee * COLS:(ee + 1) * COLS, g * LANE:(g + 1) * LANE]
                    first, second = pack_half(v[0:8], v[8:16], lane_lo)
                    usend[s0] = first
                    usend[s0 + 4] = second
        for qq, target in q_peers:
            send(usend.at[qq], urecv.at[slot, q], S_URS + layer, target)
        urecv[slot, q] = usend[q]

    def next_users(layer):
        wait_recv(urecv.at[layer % 2, pl.ds(0, OTHERS)], S_URS + layer)
        return jnp.sum(urecv[layer % 2], axis=0).astype(BF16)

    def next_items(layer):
        slot = layer % 2
        wait_recv(irecv.at[slot], S_IRS + layer)
        return ((isend[0] + irecv[slot, 0]) + (irecv[slot, 1] + irecv[slot, 2])).astype(BF16)

    for layer in range(NUM_LAYERS - 1):
        item_partials(layer)
        user_partials(layer)
        user_next = next_users(layer)
        uag[layer + 1, q] = user_next
        send_uag(layer + 1)
        acc_u = acc_u + user_next.astype(F32)
        iag[(layer + 1) % 2, pl.ds(x * 4, 4)] = next_items(layer)
        send_iag(layer + 1)
        for j in (2, 1, 3):
            send(iag.at[(layer + 1) % 2, x * 4 + es[j]], ib.at[layer, e], S_FIN + layer, device(r, c, es[j]))
        ib[layer, e] = iag[(layer + 1) % 2, x * 4 + e]

    final = NUM_LAYERS - 1
    item_partials(final)
    frecv[x * 4 + e] = isend[0, e]
    user_partials(final)
    for layer in range(final):
        wait_recv(ib.at[layer, pl.ds(0, 3)], S_FIN + layer)
    item_sums = []
    for s in range(4):
        item_sum = it_v[:, s * CHUNK:(s + 1) * CHUNK].astype(F32)
        for layer in range(final):
            item_sum = item_sum + ib[layer, s].astype(F32)
        item_sums.append(item_sum)
    acc_u = acc_u + next_users(final).astype(F32)
    fin_u = (acc_u / (NUM_LAYERS + 1)).astype(BF16)
    eu[b] = fin_u
    for _, target in b_peers:
        send(eu.at[b], eu.at[b], S_EU, target)
    fin_u = fin_u.astype(F32)
    ou_ref[...] = jnp.concatenate([fin_u[:, 0:EMB], pltpu.roll(fin_u, EMB, 1)[:, 0:EMB]], axis=0).astype(BF16)
    wait_recv(frecv.at[pl.ds(0, 15)], S_IRS + final)
    for s in range(4):
        item_next = ((frecv[s] + frecv[4 + s]) + (frecv[4 * 2 + s] + frecv[4 * 3 + s])).astype(BF16)
        fin[s] = ((item_sums[s] + item_next.astype(F32)) / (NUM_LAYERS + 1)).astype(BF16)
    for h in range(8):
        wmat[h * COLS:(h + 1) * COLS, :] = fin[h // 2, :, (h % 2) * USERS:(h % 2 + 1) * USERS]
    first_item = (c * 8 + r) * ITEMS

    for d in (4, 3, 5, 2, 6, 1, 7, 0):
        row = lax.rem(r + d, 8)
        ids = tr_ref[:, pl.ds(pl.multiple_of(row * CHUNK, CHUNK), CHUNK)] - first_item
        diff = pick_rows(wmat[...], ids[1:2]) - pick_rows(wmat[...], ids[2:3])
        for g in range(4):
            dsend[row * 4 + g] = diff[:, g * LANE:(g + 1) * LANE]
        for j in (2, 1, 3, 0):
            if d or j:
                send(dsend.at[row * 4 + cs[j]], drecv.at[b], S_D, device(row, cs[j], e))
    drecv[b] = dsend[b]
    wait_recv(eu.at[pl.ds(0, OTHERS)], S_EU)
    for g in range(COLS):
        top, bot = unpack_half(eu[2 * g].astype(F32), eu[2 * g + 1].astype(F32), lane_lo)
        umat[g // 2 * COLS:(g // 2 + 1) * COLS, g % 2 * LANE:(g % 2 + 1) * LANE] = jnp.concatenate([top, bot], axis=0).astype(BF16)
    e_user = pick_rows(umat[...], tr_ref[0:1, pl.ds(pl.multiple_of(b * LANE, LANE), LANE)])
    wait_recv(drecv.at[pl.ds(0, OTHERS)], S_D)
    mine = e * PEERS + b
    lag[mine] = jnp.sum(e_user * jnp.sum(drecv[...], axis=0), axis=0, keepdims=True)
    for target in all_peers:
        send(lag.at[mine], lag.at[mine], S_LOSS, target)
    for s in range(4):
        oi_ref[:, s * CHUNK:(s + 1) * CHUNK] = fin[s]
    wait_send(rem, S_MASK)
    wait_send(du.at[pl.ds(0, OTHERS)], S_DU)
    wait_send(di.at[pl.ds(0, 7)], S_DI)
    for layer in range(NUM_LAYERS):
        wait_send(uag.at[layer, pl.ds(0, OTHERS)], S_UAG + layer)
        if layer == 0:
            wait_send(iag.at[0, pl.ds(0, 15)], S_IAG)
        else:
            wait_send(iag.at[layer % 2, pl.ds(0, 12)], S_IAG + layer)
    wait_send(usend.at[pl.ds(0, OTHERS)], S_URS + NUM_LAYERS - 1)
    wait_send(frecv.at[pl.ds(0, 15)], S_IRS + final)
    for layer in range(final):
        wait_send(ib.at[layer, pl.ds(0, 3)], S_FIN + layer)
    wait_send(eu.at[pl.ds(0, OTHERS)], S_EU)
    wait_send(drecv.at[pl.ds(0, OTHERS)], S_D)
    wait_send(lag.at[pl.ds(0, 4 * PEERS - 1)], S_LOSS)
    wait_recv(lag.at[pl.ds(0, 4 * PEERS - 1)], S_LOSS)
    for s in range(PEERS):
        ol_ref[s:s + 1, :] = (lag[s] + lag[s + PEERS]) + (lag[s + 2 * PEERS] + lag[s + 3 * PEERS])
    score = ol_ref[...]
    ol_ref[...] = jnp.maximum(-score, 0.0) + jnp.log1p(jnp.exp(-jnp.abs(score)))


def emit_kernel(ou, oi, ol, ou_ref, oi_ref, ol_ref, sems):
    copies = [pltpu.make_async_copy(a, b, sems.at[i]) for i, (a, b) in enumerate(((oi, oi_ref), (ou, ou_ref), (ol, ol_ref)))]
    for cp in copies:
        cp.start()
    for cp in copies:
        cp.wait()


def call(body, outs, in_specs, scratch, collective_id=None, vmem_mib=24, out_spec=None):
    vmem = pl.BlockSpec(memory_space=pltpu.VMEM)
    return pl.pallas_call(
        body,
        out_shape=tuple(jax.ShapeDtypeStruct(shape, dtype) for shape, dtype in outs),
        in_specs=[vmem if s is None else s for s in in_specs],
        out_specs=(out_spec or vmem,) * len(outs),
        scratch_shapes=scratch,
        compiler_params=pltpu.CompilerParams(
            collective_id=collective_id, has_side_effects=collective_id is not None,
            vmem_limit_bytes=vmem_mib * 1024 * 1024),
        name=body.__name__)


def solution(mesh):
    vm = pltpu.VMEM
    dma = pltpu.SemaphoreType.DMA

    def local_fn(mask_blk, user_sh, item_sh, triples):
        half = (4, USERS, CHUNK)
        pieces = (PEERS, 8, LANE)
        chunk = (4, COLS, CHUNK)
        own, other, du, di = call(
            load_kernel, [(half, BF16), (half, BF16), ((1, USERS), F32), ((2, 1, ITEMS), F32)],
            [pl.BlockSpec(memory_space=pl.ANY)], [vm((2,) + half, jnp.int32), dma((8,))], vmem_mib=49)(mask_blk)
        results = [((COLS, EMB), BF16), ((COLS, ITEMS), BF16), ((PEERS, LANE), F32)]
        made = call(
            main_kernel, results, [None] * 7,
            [vm(half, BF16), vm(half, BF16), vm((PEERS, 1, USERS), F32), vm((8, 1, ITEMS), F32),
             vm((NUM_LAYERS,) + pieces, BF16), vm((2, 4 * 4, COLS, CHUNK), BF16), vm(pieces, F32),
             vm((2,) + pieces, F32),
             vm((4,) + chunk, F32), vm((2, 3) + chunk, F32), vm((2, EMB, USERS), BF16),
             vm((NUM_LAYERS - 1,) + chunk, BF16), vm((4 * 4, COLS, CHUNK), F32), vm(chunk, BF16),
             vm(pieces, BF16), vm((LANE, USERS), BF16), vm((LANE, USERS), BF16), vm((PEERS, COLS, LANE), F32),
             vm((PEERS, COLS, LANE), F32), vm((4 * PEERS, 1, LANE), F32),
             dma((N_SEM,)), dma((N_SEM,))],
            0)(own, other, du, di, user_sh.T, item_sh.T, triples.T)
        out_u, out_i, loss = call(emit_kernel, results, [None] * 3, [dma((3,))], out_spec=pl.BlockSpec(memory_space=pl.ANY))(*made)
        return out_u.T, out_i.T, loss.reshape(PEERS * LANE)

    return jax.shard_map(
        local_fn, mesh=mesh,
        in_specs=(P("row", "col"), P(("row", "col"), "emb"), P(("col", "row"), "emb"), P()),
        out_specs=(P(("row", "col"), "emb"), P(("col", "row"), "emb"), P()),
        check_vma=False)
```

```python
import jax
import jax.numpy as jnp
from jax import lax
from jax.experimental import pallas as pl
from jax.experimental.pallas import tpu as pltpu
from jax.sharding import PartitionSpec as P

NUM_LAYERS = 3
MESH = pl.DeviceIdType.MESH
F32 = jnp.float32
BF16 = jnp.bfloat16
EMB = 64
COLS = 16
LANE = 128
CHUNK = 512
ITEMS = 2048
USERS = 256
PEERS = 32
OTHERS = PEERS - 1


def pack_half(top, bot, lane_lo):
    first = jnp.where(lane_lo, top, pltpu.roll(bot, EMB, 1))
    second = jnp.where(lane_lo, pltpu.roll(top, EMB, 1), bot)
    return first, second


def unpack_half(first, second, lane_lo):
    top = jnp.where(lane_lo, first, pltpu.roll(second, EMB, 1))
    bot = jnp.where(lane_lo, pltpu.roll(first, EMB, 1), second)
    return top, bot


def pick_rows(table, ids):
    n = ids.shape[1]
    low = jnp.bitwise_and(ids, USERS - 1)
    high = jnp.broadcast_to(lax.shift_right_arithmetic(ids, 8), (COLS, n))
    hot = (lax.broadcasted_iota(jnp.int32, (USERS, n), 0) == low).astype(F32).astype(BF16)
    wide = jnp.dot(table, hot, preferred_element_type=F32)
    total = jnp.zeros((COLS, n), F32)
    for blk in range(8):
        total = jnp.where(high == blk, wide[blk * COLS:(blk + 1) * COLS], total)
    return total


def place():
    e = lax.axis_index("emb")
    c = lax.axis_index("col")
    r = lax.axis_index("row")
    return e, c, r, r // 2, r % 2


def device(r, c, e):
    return (e, c, r)


class Links:
    def __init__(self, send_sem, recv_sem):
        self.send_sem = send_sem
        self.recv_sem = recv_sem

    def send(self, src, dst, phase, target):
        pltpu.make_async_remote_copy(src_ref=src, dst_ref=dst, send_sem=self.send_sem.at[phase],
                                     recv_sem=self.recv_sem.at[phase], device_id=target, device_id_type=MESH).start()

    def wait_recv(self, ref, phase):
        pltpu.make_async_copy(ref, ref, self.recv_sem.at[phase]).wait()

    def wait_send(self, ref, phase):
        pltpu.make_async_copy(ref, ref, self.send_sem.at[phase]).wait()


def greet(target):
    pl.semaphore_signal(pltpu.get_barrier_semaphore(), inc=1, device_id=target, device_id_type=MESH)


S_MASK, S_DU, S_DI, S_EU, S_D, S_LOSS, S_FIN = range(7)
S_UAG = S_FIN + NUM_LAYERS
S_IAG = S_UAG + NUM_LAYERS
S_URS = S_IAG + NUM_LAYERS
S_IRS = S_URS + NUM_LAYERS
N_SEM = S_IRS + NUM_LAYERS


def far_first(*sizes):
    offsets = [()]
    for size in sizes:
        offsets = [o + (d,) for o in offsets for d in range(size)]
    hops = lambda o: sum(min(d, n - d) for d, n in zip(o[:-1], sizes)) * 2 + o[-1]
    return sorted(offsets[1:], key=hops, reverse=True)


def main_kernel(mask_ref, ut_ref, it_ref, tri_ref, ou_ref, oi_ref, ol_ref, ut_v, it_v, tr_ref, small_sem, m_loc, other, rem, adj, du, di_own, di, uag, iag, usend, urecv, isend, irecv, utp, ib, frecv, fin,
                eu, wmat, umat, dsend, drecv, lag, load_sem, send_sem, recv_sem):
    e, c, r, x, k = place()

    def load(par, xx):
        row = 2 * xx + (k + par) % 2
        off = pl.multiple_of(row * ITEMS + e * CHUNK, CHUNK)
        return pltpu.make_async_copy(mask_ref.at[:, pl.ds(off, CHUNK)], m_loc.at[xx], load_sem.at[par, xx])

    for xx in range(4):
        load(1, xx).start()
    small = [pltpu.make_async_copy(a, v, small_sem.at[i])
             for i, (a, v) in enumerate(((ut_ref, ut_v), (it_ref, it_v), (tri_ref, tr_ref)))]
    for cp in small:
        cp.start()
    q = k * COLS + c * 4 + e
    b = r * 4 + c
    links = Links(send_sem, recv_sem)
    send, wait_recv, wait_send = links.send, links.wait_recv, links.wait_send
    es = [lax.rem(e + d, 4) for d in range(4)]
    cs = [lax.rem(c + d, 4) for d in range(4)]
    xs = [lax.rem(x + d, 4) for d in range(4)]
    ks = [k, 1 - k]
    partner = device(2 * x + ks[1], c, e)
    q_peers = [(ks[dk] * COLS + cs[dc] * 4 + es[de], device(2 * x + ks[dk], cs[dc], es[de]))
               for dc, de, dk in far_first(4, 4, 2)]
    b_peers = [((2 * xs[dx] + ks[dk]) * 4 + cs[dc], device(2 * xs[dx] + ks[dk], cs[dc], e))
               for dx, dc, dk in far_first(4, 4, 2)]
    all_peers = [device(2 * xs[dx] + ks[dk], cs[dc], es[de]) for dx, dc, de, dk in far_first(4, 4, 4, 2)]
    xz_peers = [(es[de], device(2 * xs[dx] + k, c, es[de])) for dx, de, _ in far_first(4, 4, 1)]

    for _, target in q_peers:
        greet(target)
    for dx in range(1, 4):
        for de in range(4):
            greet(device(2 * xs[dx] + k, c, es[de]))
        greet(device(2 * xs[dx] + ks[1], c, e))

    lanes = jnp.zeros((USERS, LANE), F32)
    for par in (1, 0):
        for xx in range(4):
            load(par, xx).wait()
            sums = []
            for g in range(4):
                at = slice(g * LANE, (g + 1) * LANE)
                part = m_loc[xx, :, at].astype(F32)
                (other if par else adj)[xx, :, at] = part.astype(BF16)
                lo = xx * CHUNK + g * LANE
                di_own[par, :, lo:lo + LANE] = jnp.sum(part, axis=0, keepdims=True)
                sums.append(part)
            lanes = lanes + ((sums[0] + sums[1]) + (sums[2] + sums[3]))
            if par:
                load(0, xx).start()
    ones = jnp.ones((8, LANE), BF16)
    du[q] = lax.dot_general(ones, lanes.astype(BF16), (((1,), (1,)), ((), ())), preferred_element_type=F32)[0:1]
    di[r] = di_own[0]
    pl.semaphore_wait(pltpu.get_barrier_semaphore(), OTHERS + 12 + 3)

    for _, target in q_peers:
        send(du.at[q], du.at[q], S_DU, target)
    for dx in (2, 1, 3, 0):
        for dk in range(2):
            if dx or dk:
                send(di_own.at[dk], di.at[r], S_DI, device(2 * xs[dx] + ks[dk], c, e))
    send(other, rem, S_MASK, partner)
    lane_lo = lax.broadcasted_iota(jnp.int32, (8, LANE), 1) < EMB
    for cp in small:
        cp.wait()
    user0 = ut_v[...].astype(F32)
    packed = jnp.concatenate([user0[0:8], user0[8:16]], axis=1)
    uag[0, q] = packed.astype(BF16)
    acc_u = packed

    def send_uag(layer):
        for _, target in q_peers:
            send(uag.at[layer, q], uag.at[layer, q], S_UAG + layer, target)

    def send_iag(layer):
        for j in (2, 1, 3):
            mine = iag.at[layer % 2, pl.ds(x * 4, 4)]
            send(mine, mine, S_IAG + layer, device(2 * xs[j] + k, c, e))

    for ee, target in xz_peers:
        send(it_v.at[:, pl.ds(pl.multiple_of(ee * CHUNK, CHUNK), CHUNK)], iag.at[0, x * 4 + e], S_IAG, target)
    send_uag(0)
    iag[0, x * 4 + e] = it_v[:, pl.ds(pl.multiple_of(e * CHUNK, CHUNK), CHUNK)]
    wait_recv(du.at[pl.ds(0, OTHERS)], S_DU)
    wait_recv(di.at[pl.ds(0, 7)], S_DI)

    inv_i = lax.rsqrt(jnp.maximum(jnp.sum(di[...], axis=0), 1.0))

    def build(source, target, core):
        deg = jnp.sum(du[pl.ds(core * COLS, COLS)], axis=0)
        inv_u = lax.rsqrt(jnp.maximum(deg, 1.0))
        for rc in range(2):
            rows = slice(rc * LANE, (rc + 1) * LANE)
            col = jnp.broadcast_to(inv_u[:, rows], (LANE, LANE)).T
            for xx in range(4):
                for g in range(4):
                    lanes = slice(g * LANE, (g + 1) * LANE)
                    lo = xx * CHUNK + g * LANE
                    m = source[xx, rows, lanes].astype(F32)
                    target[xx, rows, lanes] = ((col * m) * inv_i[:, lo:lo + LANE]).astype(BF16)

    build(adj, adj, ks[0])
    wait_recv(rem, S_MASK)
    build(rem, rem, ks[1])
    parts = ((adj, ks[0]), (rem, ks[1]))

    def item_partials(layer):
        slot = layer % 2
        wait_recv(uag.at[layer, pl.ds(0, OTHERS)], S_UAG + layer)
        for h, (_, core) in enumerate(parts):
            for g in range(2):
                for ee in range(4):
                    s0 = core * COLS + g * 8 + ee
                    top, bot = unpack_half(uag[layer, s0].astype(F32), uag[layer, s0 + 4].astype(F32), lane_lo)
                    both = jnp.concatenate([top, bot], axis=0).astype(BF16)
                    utp[h, ee * COLS:(ee + 1) * COLS, g * LANE:(g + 1) * LANE] = both
        if layer >= 1:
            wait_send(isend.at[pl.ds(0, 3)], S_IRS + layer - 1)
        for j in (2, 1, 3, 0):
            part = jnp.dot(utp[0], adj[xs[j]], preferred_element_type=F32)
            isend[j] = (part + jnp.dot(utp[1], rem[xs[j]], preferred_element_type=F32)).reshape(4, COLS, CHUNK)
            if j and layer + 1 < NUM_LAYERS:
                send(isend.at[j], irecv.at[slot, j - 1], S_IRS + layer, device(2 * xs[j] + k, c, e))
            elif layer + 1 == NUM_LAYERS:
                for de in (2, 1, 3, 0):
                    if j or de:
                        send(isend.at[j, es[de]], frecv.at[x * 4 + e], S_IRS + layer, device(2 * xs[j] + k, c, es[de]))

    def user_partials(layer):
        slot = layer % 2
        if layer == 0:
            wait_recv(iag.at[0, pl.ds(0, 15)], S_IAG)
        else:
            wait_recv(iag.at[slot, pl.ds(0, 12)], S_IAG + layer)
        if layer >= 1:
            wait_send(usend.at[pl.ds(0, OTHERS)], S_URS + layer - 1)
        for half, core in parts:
            part = jnp.zeros((EMB, USERS), F32)
            for xx in range(4):
                part = part + lax.dot_general(iag[slot, xx * 4:(xx + 1) * 4].reshape(EMB, CHUNK), half[xx],
                                              (((1,), (1,)), ((), ())), preferred_element_type=F32)
            for g in range(2):
                for ee in range(4):
                    s0 = core * COLS + g * 8 + ee
                    v = part[ee * COLS:(ee + 1) * COLS, g * LANE:(g + 1) * LANE]
                    first, second = pack_half(v[0:8], v[8:16], lane_lo)
                    usend[s0] = first
                    usend[s0 + 4] = second
        for qq, target in q_peers:
            send(usend.at[qq], urecv.at[slot, q], S_URS + layer, target)
        urecv[slot, q] = usend[q]

    def next_users(layer):
        wait_recv(urecv.at[layer % 2, pl.ds(0, OTHERS)], S_URS + layer)
        return jnp.sum(urecv[layer % 2], axis=0).astype(BF16)

    def next_items(layer):
        slot = layer % 2
        wait_recv(irecv.at[slot], S_IRS + layer)
        return ((isend[0] + irecv[slot, 0]) + (irecv[slot, 1] + irecv[slot, 2])).astype(BF16)

    for layer in range(NUM_LAYERS - 1):
        item_partials(layer)
        user_partials(layer)
        user_next = next_users(layer)
        uag[layer + 1, q] = user_next
        send_uag(layer + 1)
        acc_u = acc_u + user_next.astype(F32)
        iag[(layer + 1) % 2, pl.ds(x * 4, 4)] = next_items(layer)
        send_iag(layer + 1)
        for j in (2, 1, 3):
            send(iag.at[(layer + 1) % 2, x * 4 + es[j]], ib.at[layer, e], S_FIN + layer, device(r, c, es[j]))
        ib[layer, e] = iag[(layer + 1) % 2, x * 4 + e]

    final = NUM_LAYERS - 1
    item_partials(final)
    frecv[x * 4 + e] = isend[0, e]
    user_partials(final)
    for layer in range(final):
        wait_recv(ib.at[layer, pl.ds(0, 3)], S_FIN + layer)
    item_sums = []
    for s in range(4):
        item_sum = it_v[:, s * CHUNK:(s + 1) * CHUNK].astype(F32)
        for layer in range(final):
            item_sum = item_sum + ib[layer, s].astype(F32)
        item_sums.append(item_sum)
    acc_u = acc_u + next_users(final).astype(F32)
    fin_u = (acc_u / (NUM_LAYERS + 1)).astype(BF16)
    eu[b] = fin_u
    for _, target in b_peers:
        send(eu.at[b], eu.at[b], S_EU, target)
    fin_u = fin_u.astype(F32)
    ou_ref[...] = jnp.concatenate([fin_u[:, 0:EMB], pltpu.roll(fin_u, EMB, 1)[:, 0:EMB]], axis=0).astype(BF16)
    wait_recv(frecv.at[pl.ds(0, 15)], S_IRS + final)
    for s in range(4):
        item_next = ((frecv[s] + frecv[4 + s]) + (frecv[4 * 2 + s] + frecv[4 * 3 + s])).astype(BF16)
        fin[s] = ((item_sums[s] + item_next.astype(F32)) / (NUM_LAYERS + 1)).astype(BF16)
    for h in range(8):
        wmat[h * COLS:(h + 1) * COLS, :] = fin[h // 2, :, (h % 2) * USERS:(h % 2 + 1) * USERS]
    first_item = (c * 8 + r) * ITEMS

    for d in (4, 3, 5, 2, 6, 1, 7, 0):
        row = lax.rem(r + d, 8)
        ids = tr_ref[:, pl.ds(pl.multiple_of(row * CHUNK, CHUNK), CHUNK)] - first_item
        diff = pick_rows(wmat[...], ids[1:2]) - pick_rows(wmat[...], ids[2:3])
        for g in range(4):
            dsend[row * 4 + g] = diff[:, g * LANE:(g + 1) * LANE]
        for j in (2, 1, 3, 0):
            if d or j:
                send(dsend.at[row * 4 + cs[j]], drecv.at[b], S_D, device(row, cs[j], e))
    drecv[b] = dsend[b]
    wait_recv(eu.at[pl.ds(0, OTHERS)], S_EU)
    for g in range(COLS):
        top, bot = unpack_half(eu[2 * g].astype(F32), eu[2 * g + 1].astype(F32), lane_lo)
        umat[g // 2 * COLS:(g // 2 + 1) * COLS, g % 2 * LANE:(g % 2 + 1) * LANE] = jnp.concatenate([top, bot], axis=0).astype(BF16)
    e_user = pick_rows(umat[...], tr_ref[0:1, pl.ds(pl.multiple_of(b * LANE, LANE), LANE)])
    wait_recv(drecv.at[pl.ds(0, OTHERS)], S_D)
    mine = e * PEERS + b
    lag[mine] = jnp.sum(e_user * jnp.sum(drecv[...], axis=0), axis=0, keepdims=True)
    for target in all_peers:
        send(lag.at[mine], lag.at[mine], S_LOSS, target)
    for s in range(4):
        oi_ref[:, s * CHUNK:(s + 1) * CHUNK] = fin[s]
    wait_send(rem, S_MASK)
    wait_send(du.at[pl.ds(0, OTHERS)], S_DU)
    wait_send(di.at[pl.ds(0, 7)], S_DI)
    for layer in range(NUM_LAYERS):
        wait_send(uag.at[layer, pl.ds(0, OTHERS)], S_UAG + layer)
        if layer == 0:
            wait_send(iag.at[0, pl.ds(0, 15)], S_IAG)
        else:
            wait_send(iag.at[layer % 2, pl.ds(0, 12)], S_IAG + layer)
    wait_send(usend.at[pl.ds(0, OTHERS)], S_URS + NUM_LAYERS - 1)
    wait_send(frecv.at[pl.ds(0, 15)], S_IRS + final)
    for layer in range(final):
        wait_send(ib.at[layer, pl.ds(0, 3)], S_FIN + layer)
    wait_send(eu.at[pl.ds(0, OTHERS)], S_EU)
    wait_send(drecv.at[pl.ds(0, OTHERS)], S_D)
    wait_send(lag.at[pl.ds(0, 4 * PEERS - 1)], S_LOSS)
    wait_recv(lag.at[pl.ds(0, 4 * PEERS - 1)], S_LOSS)
    for s in range(PEERS):
        ol_ref[s:s + 1, :] = (lag[s] + lag[s + PEERS]) + (lag[s + 2 * PEERS] + lag[s + 3 * PEERS])
    score = ol_ref[...]
    ol_ref[...] = jnp.maximum(-score, 0.0) + jnp.log1p(jnp.exp(-jnp.abs(score)))


def emit_kernel(ou, oi, ol, ou_ref, oi_ref, ol_ref, sems):
    copies = [pltpu.make_async_copy(a, b, sems.at[i]) for i, (a, b) in enumerate(((oi, oi_ref), (ou, ou_ref), (ol, ol_ref)))]
    for cp in copies:
        cp.start()
    for cp in copies:
        cp.wait()


def call(body, outs, in_specs, scratch, collective_id=None, vmem_mib=24, out_spec=None):
    vmem = pl.BlockSpec(memory_space=pltpu.VMEM)
    return pl.pallas_call(
        body,
        out_shape=tuple(jax.ShapeDtypeStruct(shape, dtype) for shape, dtype in outs),
        in_specs=[vmem if s is None else s for s in in_specs],
        out_specs=(out_spec or vmem,) * len(outs),
        scratch_shapes=scratch,
        compiler_params=pltpu.CompilerParams(
            collective_id=collective_id, has_side_effects=collective_id is not None,
            vmem_limit_bytes=vmem_mib * 1024 * 1024),
        name=body.__name__)


def solution(mesh):
    vm = pltpu.VMEM
    dma = pltpu.SemaphoreType.DMA

    def local_fn(mask_blk, user_sh, item_sh, triples):
        half = (4, USERS, CHUNK)
        pieces = (PEERS, 8, LANE)
        chunk = (4, COLS, CHUNK)
        results = [((COLS, EMB), BF16), ((COLS, ITEMS), BF16), ((PEERS, LANE), F32)]
        made = call(
            main_kernel, results, [pl.BlockSpec(memory_space=pl.ANY)] * 4,
            [vm((COLS, EMB), BF16), vm((COLS, ITEMS), BF16), vm((3, PEERS * LANE), jnp.int32), dma((3,)),
             vm(half, jnp.int32), vm(half, BF16), vm(half, BF16), vm(half, BF16), vm((PEERS, 1, USERS), F32),
             vm((2, 1, ITEMS), F32), vm((8, 1, ITEMS), F32),
             vm((NUM_LAYERS,) + pieces, BF16), vm((2, 4 * 4, COLS, CHUNK), BF16), vm(pieces, F32),
             vm((2,) + pieces, F32),
             vm((4,) + chunk, F32), vm((2, 3) + chunk, F32), vm((2, EMB, USERS), BF16),
             vm((NUM_LAYERS - 1,) + chunk, BF16), vm((4 * 4, COLS, CHUNK), F32), vm(chunk, BF16),
             vm(pieces, BF16), vm((LANE, USERS), BF16), vm((LANE, USERS), BF16), vm((PEERS, COLS, LANE), F32),
             vm((PEERS, COLS, LANE), F32), vm((4 * PEERS, 1, LANE), F32),
             dma((2, 4)), dma((N_SEM,)), dma((N_SEM,))],
            0, vmem_mib=40)(*(pltpu.with_memory_space_constraint(a, pltpu.HBM) for a in (mask_blk, user_sh.T, item_sh.T, triples.T)))
        out_u, out_i, loss = call(emit_kernel, results, [None] * 3, [dma((3,))], out_spec=pl.BlockSpec(memory_space=pl.ANY))(*made)
        return out_u.T, out_i.T, loss.reshape(PEERS * LANE)

    return jax.shard_map(
        local_fn, mesh=mesh,
        in_specs=(P("row", "col"), P(("row", "col"), "emb"), P(("col", "row"), "emb"), P()),
        out_specs=(P(("row", "col"), "emb"), P(("col", "row"), "emb"), P()),
        check_vma=False)
```

```python
import jax
import jax.numpy as jnp
from jax import lax
from jax.experimental import pallas as pl
from jax.experimental.pallas import tpu as pltpu
from jax.sharding import PartitionSpec as P

NUM_LAYERS = 3
MESH = pl.DeviceIdType.MESH
F32 = jnp.float32
BF16 = jnp.bfloat16
EMB = 64
COLS = 16
LANE = 128
CHUNK = 512
ITEMS = 2048
USERS = 256
PEERS = 32
OTHERS = PEERS - 1


def pack_half(top, bot, lane_lo):
    first = jnp.where(lane_lo, top, pltpu.roll(bot, EMB, 1))
    second = jnp.where(lane_lo, pltpu.roll(top, EMB, 1), bot)
    return first, second


def unpack_half(first, second, lane_lo):
    top = jnp.where(lane_lo, first, pltpu.roll(second, EMB, 1))
    bot = jnp.where(lane_lo, pltpu.roll(first, EMB, 1), second)
    return top, bot


def pick_rows(table, ids):
    n = ids.shape[1]
    low = jnp.bitwise_and(ids, USERS - 1)
    high = jnp.broadcast_to(lax.shift_right_arithmetic(ids, 8), (COLS, n))
    hot = (lax.broadcasted_iota(jnp.int32, (USERS, n), 0) == low).astype(F32).astype(BF16)
    wide = jnp.dot(table, hot, preferred_element_type=F32)
    total = jnp.zeros((COLS, n), F32)
    for blk in range(8):
        total = jnp.where(high == blk, wide[blk * COLS:(blk + 1) * COLS], total)
    return total


def place():
    e = lax.axis_index("emb")
    c = lax.axis_index("col")
    r = lax.axis_index("row")
    return e, c, r, r // 2, r % 2


def device(r, c, e):
    return (e, c, r)


class Links:
    def __init__(self, send_sem, recv_sem):
        self.send_sem = send_sem
        self.recv_sem = recv_sem

    def send(self, src, dst, phase, target):
        pltpu.make_async_remote_copy(src_ref=src, dst_ref=dst, send_sem=self.send_sem.at[phase],
                                     recv_sem=self.recv_sem.at[phase], device_id=target, device_id_type=MESH).start()

    def wait_recv(self, ref, phase):
        pltpu.make_async_copy(ref, ref, self.recv_sem.at[phase]).wait()

    def wait_send(self, ref, phase):
        pltpu.make_async_copy(ref, ref, self.send_sem.at[phase]).wait()


def greet(target):
    pl.semaphore_signal(pltpu.get_barrier_semaphore(), inc=1, device_id=target, device_id_type=MESH)


S_MASK, S_DU, S_DI, S_EU, S_D, S_LOSS, S_FIN = range(7)
S_UAG = S_FIN + NUM_LAYERS
S_IAG = S_UAG + NUM_LAYERS
S_URS = S_IAG + 4 * NUM_LAYERS
S_IRS = S_URS + NUM_LAYERS
N_SEM = S_IRS + NUM_LAYERS


def far_first(*sizes):
    offsets = [()]
    for size in sizes:
        offsets = [o + (d,) for o in offsets for d in range(size)]
    hops = lambda o: sum(min(d, n - d) for d, n in zip(o[:-1], sizes)) * 2 + o[-1]
    return sorted(offsets[1:], key=hops, reverse=True)


def main_kernel(mask_ref, ut_ref, it_ref, tri_ref, ou_ref, oi_ref, ol_ref, ut_v, it_v, tr_ref, small_sem, m_loc, other, rem, adj, du, di_own, di, uag, iag, usend, urecv, isend, irecv, utp, ib, frecv, fin,
                eu, wmat, umat, dsend, drecv, lag, load_sem, send_sem, recv_sem):
    e, c, r, x, k = place()

    def load(par, xx):
        row = 2 * xx + (k + par) % 2
        off = pl.multiple_of(row * ITEMS + e * CHUNK, CHUNK)
        return pltpu.make_async_copy(mask_ref.at[:, pl.ds(off, CHUNK)], m_loc.at[xx], load_sem.at[par, xx])

    for xx in range(4):
        load(1, xx).start()
    small = [pltpu.make_async_copy(a, v, small_sem.at[i])
             for i, (a, v) in enumerate(((ut_ref, ut_v), (it_ref, it_v), (tri_ref, tr_ref)))]
    for cp in small:
        cp.start()
    q = k * COLS + c * 4 + e
    b = r * 4 + c
    links = Links(send_sem, recv_sem)
    send, wait_recv, wait_send = links.send, links.wait_recv, links.wait_send
    es = [lax.rem(e + d, 4) for d in range(4)]
    cs = [lax.rem(c + d, 4) for d in range(4)]
    xs = [lax.rem(x + d, 4) for d in range(4)]
    ks = [k, 1 - k]
    partner = device(2 * x + ks[1], c, e)
    q_peers = [(ks[dk] * COLS + cs[dc] * 4 + es[de], device(2 * x + ks[dk], cs[dc], es[de]))
               for dc, de, dk in far_first(4, 4, 2)]
    b_peers = [((2 * xs[dx] + ks[dk]) * 4 + cs[dc], device(2 * xs[dx] + ks[dk], cs[dc], e))
               for dx, dc, dk in far_first(4, 4, 2)]
    all_peers = [device(2 * xs[dx] + ks[dk], cs[dc], es[de]) for dx, dc, de, dk in far_first(4, 4, 4, 2)]
    xz_peers = [(es[de], device(2 * xs[dx] + k, c, es[de])) for dx, de, _ in far_first(4, 4, 1)]

    for _, target in q_peers:
        greet(target)
    for dx in range(1, 4):
        for de in range(4):
            greet(device(2 * xs[dx] + k, c, es[de]))
        greet(device(2 * xs[dx] + ks[1], c, e))

    lanes = jnp.zeros((USERS, LANE), F32)
    for par in (1, 0):
        for xx in range(4):
            load(par, xx).wait()
            sums = []
            for g in range(4):
                at = slice(g * LANE, (g + 1) * LANE)
                part = m_loc[xx, :, at].astype(F32)
                (other if par else adj)[xx, :, at] = part.astype(BF16)
                lo = xx * CHUNK + g * LANE
                di_own[par, :, lo:lo + LANE] = jnp.sum(part, axis=0, keepdims=True)
                sums.append(part)
            lanes = lanes + ((sums[0] + sums[1]) + (sums[2] + sums[3]))
            if par:
                load(0, xx).start()
    ones = jnp.ones((8, LANE), BF16)
    du[q] = lax.dot_general(ones, lanes.astype(BF16), (((1,), (1,)), ((), ())), preferred_element_type=F32)[0:1]
    di[r] = di_own[0]
    pl.semaphore_wait(pltpu.get_barrier_semaphore(), OTHERS + 12 + 3)

    for _, target in q_peers:
        send(du.at[q], du.at[q], S_DU, target)
    for dx in (2, 1, 3, 0):
        for dk in range(2):
            if dx or dk:
                send(di_own.at[dk], di.at[r], S_DI, device(2 * xs[dx] + ks[dk], c, e))
    send(other, rem, S_MASK, partner)
    lane_lo = lax.broadcasted_iota(jnp.int32, (8, LANE), 1) < EMB
    for cp in small:
        cp.wait()
    user0 = ut_v[...].astype(F32)
    packed = jnp.concatenate([user0[0:8], user0[8:16]], axis=1)
    uag[0, q] = packed.astype(BF16)
    acc_u = packed

    def send_uag(layer):
        for _, target in q_peers:
            send(uag.at[layer, q], uag.at[layer, q], S_UAG + layer, target)

    def send_iag(layer):
        for j in (1, 3, 2):
            mine = iag.at[layer % 2, pl.ds(x * 4, 4)]
            send(mine, mine, S_IAG + 4 * layer + j, device(2 * xs[j] + k, c, e))

    for ee, target in xz_peers:
        send(it_v.at[:, pl.ds(pl.multiple_of(ee * CHUNK, CHUNK), CHUNK)], iag.at[0, x * 4 + e], S_IAG, target)
    send_uag(0)
    iag[0, x * 4 + e] = it_v[:, pl.ds(pl.multiple_of(e * CHUNK, CHUNK), CHUNK)]
    wait_recv(du.at[pl.ds(0, OTHERS)], S_DU)
    wait_recv(di.at[pl.ds(0, 7)], S_DI)

    inv_i = lax.rsqrt(jnp.maximum(jnp.sum(di[...], axis=0), 1.0))

    def build(source, target, core):
        deg = jnp.sum(du[pl.ds(core * COLS, COLS)], axis=0)
        inv_u = lax.rsqrt(jnp.maximum(deg, 1.0))
        for rc in range(2):
            rows = slice(rc * LANE, (rc + 1) * LANE)
            col = jnp.broadcast_to(inv_u[:, rows], (LANE, LANE)).T
            for xx in range(4):
                for g in range(4):
                    lanes = slice(g * LANE, (g + 1) * LANE)
                    lo = xx * CHUNK + g * LANE
                    m = source[xx, rows, lanes].astype(F32)
                    target[xx, rows, lanes] = ((col * m) * inv_i[:, lo:lo + LANE]).astype(BF16)

    build(adj, adj, ks[0])
    wait_recv(rem, S_MASK)
    build(rem, rem, ks[1])
    parts = ((adj, ks[0]), (rem, ks[1]))

    def item_partials(layer):
        slot = layer % 2
        wait_recv(uag.at[layer, pl.ds(0, OTHERS)], S_UAG + layer)
        for h, (_, core) in enumerate(parts):
            for g in range(2):
                for ee in range(4):
                    s0 = core * COLS + g * 8 + ee
                    top, bot = unpack_half(uag[layer, s0].astype(F32), uag[layer, s0 + 4].astype(F32), lane_lo)
                    both = jnp.concatenate([top, bot], axis=0).astype(BF16)
                    utp[h, ee * COLS:(ee + 1) * COLS, g * LANE:(g + 1) * LANE] = both
        if layer >= 1:
            wait_send(isend.at[pl.ds(0, 3)], S_IRS + layer - 1)
        for j in (1, 3, 2, 0):
            part = jnp.dot(utp[0], adj[xs[j]], preferred_element_type=F32)
            isend[j] = (part + jnp.dot(utp[1], rem[xs[j]], preferred_element_type=F32)).reshape(4, COLS, CHUNK)
            if j and layer + 1 < NUM_LAYERS:
                send(isend.at[j], irecv.at[slot, j - 1], S_IRS + layer, device(2 * xs[j] + k, c, e))
            elif layer + 1 == NUM_LAYERS:
                for de in (2, 1, 3, 0):
                    if j or de:
                        send(isend.at[j, es[de]], frecv.at[x * 4 + e], S_IRS + layer, device(2 * xs[j] + k, c, es[de]))

    def user_partials(layer):
        slot = layer % 2
        if layer == 0:
            wait_recv(iag.at[0, pl.ds(0, 15)], S_IAG)
        if layer >= 1:
            wait_send(usend.at[pl.ds(0, OTHERS)], S_URS + layer - 1)
        made = [jnp.zeros((EMB, USERS), F32) for _ in parts]
        for j in (0, 1, 3, 2):
            if layer and j:
                wait_recv(iag.at[slot, pl.ds(0, 4)], S_IAG + 4 * layer + 4 - j)
            panel = iag[slot, pl.ds(xs[j] * 4, 4)].reshape(EMB, CHUNK)
            for h, (half, _) in enumerate(parts):
                made[h] = made[h] + lax.dot_general(panel, half[xs[j]], (((1,), (1,)), ((), ())), preferred_element_type=F32)
        for part, (_, core) in zip(made, parts):
            for g in range(2):
                for ee in range(4):
                    s0 = core * COLS + g * 8 + ee
                    v = part[ee * COLS:(ee + 1) * COLS, g * LANE:(g + 1) * LANE]
                    first, second = pack_half(v[0:8], v[8:16], lane_lo)
                    usend[s0] = first
                    usend[s0 + 4] = second
        for qq, target in q_peers:
            send(usend.at[qq], urecv.at[slot, q], S_URS + layer, target)
        urecv[slot, q] = usend[q]

    def next_users(layer):
        wait_recv(urecv.at[layer % 2, pl.ds(0, OTHERS)], S_URS + layer)
        return jnp.sum(urecv[layer % 2], axis=0).astype(BF16)

    def next_items(layer):
        slot = layer % 2
        wait_recv(irecv.at[slot], S_IRS + layer)
        return ((isend[0] + irecv[slot, 0]) + (irecv[slot, 1] + irecv[slot, 2])).astype(BF16)

    for layer in range(NUM_LAYERS - 1):
        item_partials(layer)
        user_partials(layer)
        user_next = next_users(layer)
        uag[layer + 1, q] = user_next
        send_uag(layer + 1)
        acc_u = acc_u + user_next.astype(F32)
        iag[(layer + 1) % 2, pl.ds(x * 4, 4)] = next_items(layer)
        send_iag(layer + 1)
        for j in (2, 1, 3):
            send(iag.at[(layer + 1) % 2, x * 4 + es[j]], ib.at[layer, e], S_FIN + layer, device(r, c, es[j]))
        ib[layer, e] = iag[(layer + 1) % 2, x * 4 + e]

    final = NUM_LAYERS - 1
    item_partials(final)
    frecv[x * 4 + e] = isend[0, e]
    user_partials(final)
    for layer in range(final):
        wait_recv(ib.at[layer, pl.ds(0, 3)], S_FIN + layer)
    item_sums = []
    for s in range(4):
        item_sum = it_v[:, s * CHUNK:(s + 1) * CHUNK].astype(F32)
        for layer in range(final):
            item_sum = item_sum + ib[layer, s].astype(F32)
        item_sums.append(item_sum)
    acc_u = acc_u + next_users(final).astype(F32)
    fin_u = (acc_u / (NUM_LAYERS + 1)).astype(BF16)
    eu[b] = fin_u
    for _, target in b_peers:
        send(eu.at[b], eu.at[b], S_EU, target)
    fin_u = fin_u.astype(F32)
    ou_ref[...] = jnp.concatenate([fin_u[:, 0:EMB], pltpu.roll(fin_u, EMB, 1)[:, 0:EMB]], axis=0).astype(BF16)
    wait_recv(frecv.at[pl.ds(0, 15)], S_IRS + final)
    for s in range(4):
        item_next = ((frecv[s] + frecv[4 + s]) + (frecv[4 * 2 + s] + frecv[4 * 3 + s])).astype(BF16)
        fin[s] = ((item_sums[s] + item_next.astype(F32)) / (NUM_LAYERS + 1)).astype(BF16)
    for h in range(8):
        wmat[h * COLS:(h + 1) * COLS, :] = fin[h // 2, :, (h % 2) * USERS:(h % 2 + 1) * USERS]
    first_item = (c * 8 + r) * ITEMS

    for d in (4, 3, 5, 2, 6, 1, 7, 0):
        row = lax.rem(r + d, 8)
        ids = tr_ref[:, pl.ds(pl.multiple_of(row * CHUNK, CHUNK), CHUNK)] - first_item
        diff = pick_rows(wmat[...], ids[1:2]) - pick_rows(wmat[...], ids[2:3])
        for g in range(4):
            dsend[row * 4 + g] = diff[:, g * LANE:(g + 1) * LANE]
        for j in (2, 1, 3, 0):
            if d or j:
                send(dsend.at[row * 4 + cs[j]], drecv.at[b], S_D, device(row, cs[j], e))
    drecv[b] = dsend[b]
    wait_recv(eu.at[pl.ds(0, OTHERS)], S_EU)
    for g in range(COLS):
        top, bot = unpack_half(eu[2 * g].astype(F32), eu[2 * g + 1].astype(F32), lane_lo)
        umat[g // 2 * COLS:(g // 2 + 1) * COLS, g % 2 * LANE:(g % 2 + 1) * LANE] = jnp.concatenate([top, bot], axis=0).astype(BF16)
    e_user = pick_rows(umat[...], tr_ref[0:1, pl.ds(pl.multiple_of(b * LANE, LANE), LANE)])
    wait_recv(drecv.at[pl.ds(0, OTHERS)], S_D)
    mine = e * PEERS + b
    lag[mine] = jnp.sum(e_user * jnp.sum(drecv[...], axis=0), axis=0, keepdims=True)
    for target in all_peers:
        send(lag.at[mine], lag.at[mine], S_LOSS, target)
    for s in range(4):
        oi_ref[:, s * CHUNK:(s + 1) * CHUNK] = fin[s]
    wait_send(rem, S_MASK)
    wait_send(du.at[pl.ds(0, OTHERS)], S_DU)
    wait_send(di.at[pl.ds(0, 7)], S_DI)
    for layer in range(NUM_LAYERS):
        wait_send(uag.at[layer, pl.ds(0, OTHERS)], S_UAG + layer)
        if layer == 0:
            wait_send(iag.at[0, pl.ds(0, 15)], S_IAG)
        else:
            for j in range(1, 4):
                wait_send(iag.at[layer % 2, pl.ds(0, 4)], S_IAG + 4 * layer + j)
    wait_send(usend.at[pl.ds(0, OTHERS)], S_URS + NUM_LAYERS - 1)
    wait_send(frecv.at[pl.ds(0, 15)], S_IRS + final)
    for layer in range(final):
        wait_send(ib.at[layer, pl.ds(0, 3)], S_FIN + layer)
    wait_send(eu.at[pl.ds(0, OTHERS)], S_EU)
    wait_send(drecv.at[pl.ds(0, OTHERS)], S_D)
    wait_send(lag.at[pl.ds(0, 4 * PEERS - 1)], S_LOSS)
    wait_recv(lag.at[pl.ds(0, 4 * PEERS - 1)], S_LOSS)
    for s in range(PEERS):
        ol_ref[s:s + 1, :] = (lag[s] + lag[s + PEERS]) + (lag[s + 2 * PEERS] + lag[s + 3 * PEERS])
    score = ol_ref[...]
    ol_ref[...] = jnp.maximum(-score, 0.0) + jnp.log1p(jnp.exp(-jnp.abs(score)))


def emit_kernel(ou, oi, ol, ou_ref, oi_ref, ol_ref, sems):
    copies = [pltpu.make_async_copy(a, b, sems.at[i]) for i, (a, b) in enumerate(((oi, oi_ref), (ou, ou_ref), (ol, ol_ref)))]
    for cp in copies:
        cp.start()
    for cp in copies:
        cp.wait()


def call(body, outs, in_specs, scratch, collective_id=None, vmem_mib=24, out_spec=None):
    vmem = pl.BlockSpec(memory_space=pltpu.VMEM)
    return pl.pallas_call(
        body,
        out_shape=tuple(jax.ShapeDtypeStruct(shape, dtype) for shape, dtype in outs),
        in_specs=[vmem if s is None else s for s in in_specs],
        out_specs=(out_spec or vmem,) * len(outs),
        scratch_shapes=scratch,
        compiler_params=pltpu.CompilerParams(
            collective_id=collective_id, has_side_effects=collective_id is not None,
            vmem_limit_bytes=vmem_mib * 1024 * 1024),
        name=body.__name__)


def solution(mesh):
    vm = pltpu.VMEM
    dma = pltpu.SemaphoreType.DMA

    def local_fn(mask_blk, user_sh, item_sh, triples):
        half = (4, USERS, CHUNK)
        pieces = (PEERS, 8, LANE)
        chunk = (4, COLS, CHUNK)
        results = [((COLS, EMB), BF16), ((COLS, ITEMS), BF16), ((PEERS, LANE), F32)]
        made = call(
            main_kernel, results, [pl.BlockSpec(memory_space=pl.ANY)] * 4,
            [vm((COLS, EMB), BF16), vm((COLS, ITEMS), BF16), vm((3, PEERS * LANE), jnp.int32), dma((3,)),
             vm(half, jnp.int32), vm(half, BF16), vm(half, BF16), vm(half, BF16), vm((PEERS, 1, USERS), F32),
             vm((2, 1, ITEMS), F32), vm((8, 1, ITEMS), F32),
             vm((NUM_LAYERS,) + pieces, BF16), vm((2, 4 * 4, COLS, CHUNK), BF16), vm(pieces, F32),
             vm((2,) + pieces, F32),
             vm((4,) + chunk, F32), vm((2, 3) + chunk, F32), vm((2, EMB, USERS), BF16),
             vm((NUM_LAYERS - 1,) + chunk, BF16), vm((4 * 4, COLS, CHUNK), F32), vm(chunk, BF16),
             vm(pieces, BF16), vm((LANE, USERS), BF16), vm((LANE, USERS), BF16), vm((PEERS, COLS, LANE), F32),
             vm((PEERS, COLS, LANE), F32), vm((4 * PEERS, 1, LANE), F32),
             dma((2, 4)), dma((N_SEM,)), dma((N_SEM,))],
            0, vmem_mib=40)(*(pltpu.with_memory_space_constraint(a, pltpu.HBM) for a in (mask_blk, user_sh.T, item_sh.T, triples.T)))
        out_u, out_i, loss = call(emit_kernel, results, [None] * 3, [dma((3,))], out_spec=pl.BlockSpec(memory_space=pl.ANY))(*made)
        return out_u.T, out_i.T, loss.reshape(PEERS * LANE)

    return jax.shard_map(
        local_fn, mesh=mesh,
        in_specs=(P("row", "col"), P(("row", "col"), "emb"), P(("col", "row"), "emb"), P()),
        out_specs=(P(("row", "col"), "emb"), P(("col", "row"), "emb"), P()),
        check_vma=False)
```

```python
import jax
import jax.numpy as jnp
from jax import lax
from jax.experimental import pallas as pl
from jax.experimental.pallas import tpu as pltpu
from jax.sharding import PartitionSpec as P

NUM_LAYERS = 3
MESH = pl.DeviceIdType.MESH
F32 = jnp.float32
BF16 = jnp.bfloat16
EMB = 64
COLS = 16
LANE = 128
CHUNK = 512
ITEMS = 2048
USERS = 256
PEERS = 32
OTHERS = PEERS - 1


def pack_half(top, bot, lane_lo):
    first = jnp.where(lane_lo, top, pltpu.roll(bot, EMB, 1))
    second = jnp.where(lane_lo, pltpu.roll(top, EMB, 1), bot)
    return first, second


def unpack_half(first, second, lane_lo):
    top = jnp.where(lane_lo, first, pltpu.roll(second, EMB, 1))
    bot = jnp.where(lane_lo, pltpu.roll(first, EMB, 1), second)
    return top, bot


def pick_rows(table, ids):
    n = ids.shape[1]
    low = jnp.bitwise_and(ids, USERS - 1)
    high = jnp.broadcast_to(lax.shift_right_arithmetic(ids, 8), (COLS, n))
    lanes = lax.broadcasted_iota(jnp.int32, (USERS, n), 0).astype(F32).astype(BF16)
    same = lanes == low.astype(F32).astype(BF16)
    hot = jnp.where(same, jnp.ones((), BF16), jnp.zeros((), BF16))
    wide = jnp.dot(table, hot, preferred_element_type=F32)
    total = jnp.zeros((COLS, n), F32)
    for blk in range(8):
        total = jnp.where(high == blk, wide[blk * COLS:(blk + 1) * COLS], total)
    return total


def place():
    e = lax.axis_index("emb")
    c = lax.axis_index("col")
    r = lax.axis_index("row")
    return e, c, r, r // 2, r % 2


def device(r, c, e):
    return (e, c, r)


class Links:
    def __init__(self, send_sem, recv_sem):
        self.send_sem = send_sem
        self.recv_sem = recv_sem

    def send(self, src, dst, phase, target):
        pltpu.make_async_remote_copy(src_ref=src, dst_ref=dst, send_sem=self.send_sem.at[phase],
                                     recv_sem=self.recv_sem.at[phase], device_id=target, device_id_type=MESH).start()

    def wait_recv(self, ref, phase):
        pltpu.make_async_copy(ref, ref, self.recv_sem.at[phase]).wait()

    def wait_send(self, ref, phase):
        pltpu.make_async_copy(ref, ref, self.send_sem.at[phase]).wait()


def greet(target):
    pl.semaphore_signal(pltpu.get_barrier_semaphore(), inc=1, device_id=target, device_id_type=MESH)


S_MASK, S_DU, S_DI, S_EU, S_D, S_LOSS, S_FIN = range(7)
S_UAG = S_FIN + NUM_LAYERS
S_IAG = S_UAG + NUM_LAYERS
S_URS = S_IAG + 4 * NUM_LAYERS
S_IRS = S_URS + NUM_LAYERS
N_SEM = S_IRS + NUM_LAYERS


def far_first(*sizes):
    offsets = [()]
    for size in sizes:
        offsets = [o + (d,) for o in offsets for d in range(size)]
    hops = lambda o: sum(min(d, n - d) for d, n in zip(o[:-1], sizes)) * 2 + o[-1]
    return sorted(offsets[1:], key=hops, reverse=True)


def main_kernel(mask_ref, ut_ref, it_ref, tri_ref, ou_ref, oi_ref, ol_ref, ut_v, it_v, tr_ref, small_sem, m_loc, other, rem, adj, du, di_own, di, uag, iag, usend, urecv, isend, irecv, utp, ib, frecv, fin,
                eu, wmat, umat, dsend, drecv, lag, load_sem, send_sem, recv_sem):
    e, c, r, x, k = place()

    def load(par, xx):
        row = 2 * xx + (k + par) % 2
        off = pl.multiple_of(row * ITEMS + e * CHUNK, CHUNK)
        return pltpu.make_async_copy(mask_ref.at[:, pl.ds(off, CHUNK)], m_loc.at[xx], load_sem.at[par, xx])

    for xx in range(4):
        load(1, xx).start()
    small = [pltpu.make_async_copy(a, v, small_sem.at[i])
             for i, (a, v) in enumerate(((ut_ref, ut_v), (it_ref, it_v), (tri_ref, tr_ref)))]
    for cp in small:
        cp.start()
    q = k * COLS + c * 4 + e
    b = r * 4 + c
    links = Links(send_sem, recv_sem)
    send, wait_recv, wait_send = links.send, links.wait_recv, links.wait_send
    es = [lax.rem(e + d, 4) for d in range(4)]
    cs = [lax.rem(c + d, 4) for d in range(4)]
    xs = [lax.rem(x + d, 4) for d in range(4)]
    ks = [k, 1 - k]
    partner = device(2 * x + ks[1], c, e)
    q_peers = [(ks[dk] * COLS + cs[dc] * 4 + es[de], device(2 * x + ks[dk], cs[dc], es[de]))
               for dc, de, dk in far_first(4, 4, 2)]
    b_peers = [((2 * xs[dx] + ks[dk]) * 4 + cs[dc], device(2 * xs[dx] + ks[dk], cs[dc], e))
               for dx, dc, dk in far_first(4, 4, 2)]
    all_peers = [device(2 * xs[dx] + ks[dk], cs[dc], es[de]) for dx, dc, de, dk in far_first(4, 4, 4, 2)]
    xz_peers = [(es[de], device(2 * xs[dx] + k, c, es[de])) for dx, de, _ in far_first(4, 4, 1)]

    for _, target in q_peers:
        greet(target)
    for dx in range(1, 4):
        for de in range(4):
            greet(device(2 * xs[dx] + k, c, es[de]))
        greet(device(2 * xs[dx] + ks[1], c, e))

    lanes = jnp.zeros((USERS, LANE), F32)
    for par in (1, 0):
        for xx in range(4):
            load(par, xx).wait()
            sums = []
            for g in range(4):
                at = slice(g * LANE, (g + 1) * LANE)
                part = m_loc[xx, :, at].astype(F32)
                (other if par else adj)[xx, :, at] = part.astype(BF16)
                lo = xx * CHUNK + g * LANE
                di_own[par, :, lo:lo + LANE] = jnp.sum(part, axis=0, keepdims=True)
                sums.append(part)
            lanes = lanes + ((sums[0] + sums[1]) + (sums[2] + sums[3]))
            if par:
                load(0, xx).start()
    ones = jnp.ones((8, LANE), BF16)
    du[q] = lax.dot_general(ones, lanes.astype(BF16), (((1,), (1,)), ((), ())), preferred_element_type=F32)[0:1]
    di[r] = di_own[0]
    pl.semaphore_wait(pltpu.get_barrier_semaphore(), OTHERS + 12 + 3)

    for _, target in q_peers:
        send(du.at[q], du.at[q], S_DU, target)
    for dx in (2, 1, 3, 0):
        for dk in range(2):
            if dx or dk:
                send(di_own.at[dk], di.at[r], S_DI, device(2 * xs[dx] + ks[dk], c, e))
    send(other, rem, S_MASK, partner)
    lane_lo = lax.broadcasted_iota(jnp.int32, (8, LANE), 1) < EMB
    for cp in small:
        cp.wait()
    user0 = ut_v[...].astype(F32)
    packed = jnp.concatenate([user0[0:8], user0[8:16]], axis=1)
    uag[0, q] = packed.astype(BF16)
    acc_u = packed

    def send_uag(layer):
        for _, target in q_peers:
            send(uag.at[layer, q], uag.at[layer, q], S_UAG + layer, target)

    def send_iag(layer):
        for j in (1, 3, 2):
            mine = iag.at[layer % 2, pl.ds(x * 4, 4)]
            send(mine, mine, S_IAG + 4 * layer + j, device(2 * xs[j] + k, c, e))

    for ee, target in xz_peers:
        send(it_v.at[:, pl.ds(pl.multiple_of(ee * CHUNK, CHUNK), CHUNK)], iag.at[0, x * 4 + e], S_IAG, target)
    send_uag(0)
    iag[0, x * 4 + e] = it_v[:, pl.ds(pl.multiple_of(e * CHUNK, CHUNK), CHUNK)]
    wait_recv(du.at[pl.ds(0, OTHERS)], S_DU)
    wait_recv(di.at[pl.ds(0, 7)], S_DI)

    inv_i = lax.rsqrt(jnp.maximum(jnp.sum(di[...], axis=0), 1.0))

    def build(source, target, core):
        deg = jnp.sum(du[pl.ds(core * COLS, COLS)], axis=0)
        inv_u = lax.rsqrt(jnp.maximum(deg, 1.0))
        for rc in range(2):
            rows = slice(rc * LANE, (rc + 1) * LANE)
            col = jnp.broadcast_to(inv_u[:, rows], (LANE, LANE)).T
            for xx in range(4):
                for g in range(4):
                    lanes = slice(g * LANE, (g + 1) * LANE)
                    lo = xx * CHUNK + g * LANE
                    m = source[xx, rows, lanes].astype(F32)
                    target[xx, rows, lanes] = ((col * m) * inv_i[:, lo:lo + LANE]).astype(BF16)

    build(adj, adj, ks[0])
    wait_recv(rem, S_MASK)
    build(rem, rem, ks[1])
    parts = ((adj, ks[0]), (rem, ks[1]))

    def item_partials(layer):
        slot = layer % 2
        wait_recv(uag.at[layer, pl.ds(0, OTHERS)], S_UAG + layer)
        for h, (_, core) in enumerate(parts):
            for g in range(2):
                for ee in range(4):
                    s0 = core * COLS + g * 8 + ee
                    top, bot = unpack_half(uag[layer, s0].astype(F32), uag[layer, s0 + 4].astype(F32), lane_lo)
                    both = jnp.concatenate([top, bot], axis=0).astype(BF16)
                    utp[h, ee * COLS:(ee + 1) * COLS, g * LANE:(g + 1) * LANE] = both
        if layer >= 1:
            wait_send(isend.at[pl.ds(0, 3)], S_IRS + layer - 1)
        for j in (1, 3, 2, 0):
            part = jnp.dot(utp[0], adj[xs[j]], preferred_element_type=F32)
            isend[j] = (part + jnp.dot(utp[1], rem[xs[j]], preferred_element_type=F32)).reshape(4, COLS, CHUNK)
            if j and layer + 1 < NUM_LAYERS:
                send(isend.at[j], irecv.at[slot, j - 1], S_IRS + layer, device(2 * xs[j] + k, c, e))
            elif layer + 1 == NUM_LAYERS:
                for de in (2, 1, 3, 0):
                    if j or de:
                        send(isend.at[j, es[de]], frecv.at[x * 4 + e], S_IRS + layer, device(2 * xs[j] + k, c, es[de]))

    def user_partials(layer):
        slot = layer % 2
        if layer == 0:
            wait_recv(iag.at[0, pl.ds(0, 15)], S_IAG)
        if layer >= 1:
            wait_send(usend.at[pl.ds(0, OTHERS)], S_URS + layer - 1)
        made = [jnp.zeros((EMB, USERS), F32) for _ in parts]
        for j in (0, 1, 3, 2):
            if layer and j:
                wait_recv(iag.at[slot, pl.ds(0, 4)], S_IAG + 4 * layer + 4 - j)
            panel = iag[slot, pl.ds(xs[j] * 4, 4)].reshape(EMB, CHUNK)
            for h, (half, _) in enumerate(parts):
                made[h] = made[h] + lax.dot_general(panel, half[xs[j]], (((1,), (1,)), ((), ())), preferred_element_type=F32)
        for part, (_, core) in zip(made, parts):
            for g in range(2):
                for ee in range(4):
                    s0 = core * COLS + g * 8 + ee
                    v = part[ee * COLS:(ee + 1) * COLS, g * LANE:(g + 1) * LANE]
                    first, second = pack_half(v[0:8], v[8:16], lane_lo)
                    usend[s0] = first
                    usend[s0 + 4] = second
        for qq, target in q_peers:
            send(usend.at[qq], urecv.at[slot, q], S_URS + layer, target)
        urecv[slot, q] = usend[q]

    def next_users(layer):
        wait_recv(urecv.at[layer % 2, pl.ds(0, OTHERS)], S_URS + layer)
        return jnp.sum(urecv[layer % 2], axis=0).astype(BF16)

    def next_items(layer):
        slot = layer % 2
        wait_recv(irecv.at[slot], S_IRS + layer)
        return ((isend[0] + irecv[slot, 0]) + (irecv[slot, 1] + irecv[slot, 2])).astype(BF16)

    for layer in range(NUM_LAYERS - 1):
        item_partials(layer)
        user_partials(layer)
        user_next = next_users(layer)
        uag[layer + 1, q] = user_next
        send_uag(layer + 1)
        acc_u = acc_u + user_next.astype(F32)
        iag[(layer + 1) % 2, pl.ds(x * 4, 4)] = next_items(layer)
        send_iag(layer + 1)
        for j in (2, 1, 3):
            send(iag.at[(layer + 1) % 2, x * 4 + es[j]], ib.at[layer, e], S_FIN + layer, device(r, c, es[j]))
        ib[layer, e] = iag[(layer + 1) % 2, x * 4 + e]

    final = NUM_LAYERS - 1
    item_partials(final)
    frecv[x * 4 + e] = isend[0, e]
    user_partials(final)
    for layer in range(final):
        wait_recv(ib.at[layer, pl.ds(0, 3)], S_FIN + layer)
    item_sums = []
    for s in range(4):
        item_sum = it_v[:, s * CHUNK:(s + 1) * CHUNK].astype(F32)
        for layer in range(final):
            item_sum = item_sum + ib[layer, s].astype(F32)
        item_sums.append(item_sum)
    acc_u = acc_u + next_users(final).astype(F32)
    fin_u = (acc_u / (NUM_LAYERS + 1)).astype(BF16)
    eu[b] = fin_u
    for _, target in b_peers:
        send(eu.at[b], eu.at[b], S_EU, target)
    fin_u = fin_u.astype(F32)
    ou_ref[...] = jnp.concatenate([fin_u[:, 0:EMB], pltpu.roll(fin_u, EMB, 1)[:, 0:EMB]], axis=0).astype(BF16)
    wait_recv(frecv.at[pl.ds(0, 15)], S_IRS + final)
    for s in range(4):
        item_next = ((frecv[s] + frecv[4 + s]) + (frecv[4 * 2 + s] + frecv[4 * 3 + s])).astype(BF16)
        fin[s] = ((item_sums[s] + item_next.astype(F32)) / (NUM_LAYERS + 1)).astype(BF16)
    for h in range(8):
        wmat[h * COLS:(h + 1) * COLS, :] = fin[h // 2, :, (h % 2) * USERS:(h % 2 + 1) * USERS]
    first_item = (c * 8 + r) * ITEMS

    for d in (4, 3, 5, 2, 6, 1, 7, 0):
        row = lax.rem(r + d, 8)
        ids = tr_ref[:, pl.ds(pl.multiple_of(row * CHUNK, CHUNK), CHUNK)] - first_item
        diff = pick_rows(wmat[...], ids[1:2]) - pick_rows(wmat[...], ids[2:3])
        for g in range(4):
            dsend[row * 4 + g] = diff[:, g * LANE:(g + 1) * LANE]
        for j in (2, 1, 3, 0):
            if d or j:
                send(dsend.at[row * 4 + cs[j]], drecv.at[b], S_D, device(row, cs[j], e))
    drecv[b] = dsend[b]
    wait_recv(eu.at[pl.ds(0, OTHERS)], S_EU)
    for g in range(COLS):
        top, bot = unpack_half(eu[2 * g].astype(F32), eu[2 * g + 1].astype(F32), lane_lo)
        umat[g // 2 * COLS:(g // 2 + 1) * COLS, g % 2 * LANE:(g % 2 + 1) * LANE] = jnp.concatenate([top, bot], axis=0).astype(BF16)
    e_user = pick_rows(umat[...], tr_ref[0:1, pl.ds(pl.multiple_of(b * LANE, LANE), LANE)])
    wait_recv(drecv.at[pl.ds(0, OTHERS)], S_D)
    mine = e * PEERS + b
    lag[mine] = jnp.sum(e_user * jnp.sum(drecv[...], axis=0), axis=0, keepdims=True)
    for target in all_peers:
        send(lag.at[mine], lag.at[mine], S_LOSS, target)
    for s in range(4):
        oi_ref[:, s * CHUNK:(s + 1) * CHUNK] = fin[s]
    wait_send(rem, S_MASK)
    wait_send(du.at[pl.ds(0, OTHERS)], S_DU)
    wait_send(di.at[pl.ds(0, 7)], S_DI)
    for layer in range(NUM_LAYERS):
        wait_send(uag.at[layer, pl.ds(0, OTHERS)], S_UAG + layer)
        if layer == 0:
            wait_send(iag.at[0, pl.ds(0, 15)], S_IAG)
        else:
            for j in range(1, 4):
                wait_send(iag.at[layer % 2, pl.ds(0, 4)], S_IAG + 4 * layer + j)
    wait_send(usend.at[pl.ds(0, OTHERS)], S_URS + NUM_LAYERS - 1)
    wait_send(frecv.at[pl.ds(0, 15)], S_IRS + final)
    for layer in range(final):
        wait_send(ib.at[layer, pl.ds(0, 3)], S_FIN + layer)
    wait_send(eu.at[pl.ds(0, OTHERS)], S_EU)
    wait_send(drecv.at[pl.ds(0, OTHERS)], S_D)
    wait_send(lag.at[pl.ds(0, 4 * PEERS - 1)], S_LOSS)
    wait_recv(lag.at[pl.ds(0, 4 * PEERS - 1)], S_LOSS)
    for s in range(PEERS):
        ol_ref[s:s + 1, :] = (lag[s] + lag[s + PEERS]) + (lag[s + 2 * PEERS] + lag[s + 3 * PEERS])
    score = ol_ref[...]
    ol_ref[...] = jnp.maximum(-score, 0.0) + jnp.log1p(jnp.exp(-jnp.abs(score)))


def emit_kernel(ou, oi, ol, ou_ref, oi_ref, ol_ref, sems):
    copies = [pltpu.make_async_copy(a, b, sems.at[i]) for i, (a, b) in enumerate(((oi, oi_ref), (ou, ou_ref), (ol, ol_ref)))]
    for cp in copies:
        cp.start()
    for cp in copies:
        cp.wait()


def call(body, outs, in_specs, scratch, collective_id=None, vmem_mib=24, out_spec=None):
    vmem = pl.BlockSpec(memory_space=pltpu.VMEM)
    return pl.pallas_call(
        body,
        out_shape=tuple(jax.ShapeDtypeStruct(shape, dtype) for shape, dtype in outs),
        in_specs=[vmem if s is None else s for s in in_specs],
        out_specs=(out_spec or vmem,) * len(outs),
        scratch_shapes=scratch,
        compiler_params=pltpu.CompilerParams(
            collective_id=collective_id, has_side_effects=collective_id is not None,
            vmem_limit_bytes=vmem_mib * 1024 * 1024),
        name=body.__name__)


def solution(mesh):
    vm = pltpu.VMEM
    dma = pltpu.SemaphoreType.DMA

    def local_fn(mask_blk, user_sh, item_sh, triples):
        half = (4, USERS, CHUNK)
        pieces = (PEERS, 8, LANE)
        chunk = (4, COLS, CHUNK)
        results = [((COLS, EMB), BF16), ((COLS, ITEMS), BF16), ((PEERS, LANE), F32)]
        made = call(
            main_kernel, results, [pl.BlockSpec(memory_space=pl.ANY)] * 4,
            [vm((COLS, EMB), BF16), vm((COLS, ITEMS), BF16), vm((3, PEERS * LANE), jnp.int32), dma((3,)),
             vm(half, jnp.int32), vm(half, BF16), vm(half, BF16), vm(half, BF16), vm((PEERS, 1, USERS), F32),
             vm((2, 1, ITEMS), F32), vm((8, 1, ITEMS), F32),
             vm((NUM_LAYERS,) + pieces, BF16), vm((2, 4 * 4, COLS, CHUNK), BF16), vm(pieces, F32),
             vm((2,) + pieces, F32),
             vm((4,) + chunk, F32), vm((2, 3) + chunk, F32), vm((2, EMB, USERS), BF16),
             vm((NUM_LAYERS - 1,) + chunk, BF16), vm((4 * 4, COLS, CHUNK), F32), vm(chunk, BF16),
             vm(pieces, BF16), vm((LANE, USERS), BF16), vm((LANE, USERS), BF16), vm((PEERS, COLS, LANE), F32),
             vm((PEERS, COLS, LANE), F32), vm((4 * PEERS, 1, LANE), F32),
             dma((2, 4)), dma((N_SEM,)), dma((N_SEM,))],
            0, vmem_mib=40)(*(pltpu.with_memory_space_constraint(a, pltpu.HBM) for a in (mask_blk, user_sh.T, item_sh.T, triples.T)))
        out_u, out_i, loss = call(emit_kernel, results, [None] * 3, [dma((3,))], out_spec=pl.BlockSpec(memory_space=pl.ANY))(*made)
        return out_u.T, out_i.T, loss.reshape(PEERS * LANE)

    return jax.shard_map(
        local_fn, mesh=mesh,
        in_specs=(P("row", "col"), P(("row", "col"), "emb"), P(("col", "row"), "emb"), P()),
        out_specs=(P(("row", "col"), "emb"), P(("col", "row"), "emb"), P()),
        check_vma=False)
```
